16 devices in a mesh: tp: 2 (over z), dp: 8 (over y, x, core).
Axes of the slice: x: 2, y: 2, z: 2, core: 2. Of those that a mesh axis runs over, the one named last changes fastest.
Arguments:
- hidden: bfloat16 [64, 512, 7168], P('dp')
- gain_in: float32 [7168], replicated
- gain_q: float32 [1536], replicated
- gain_kv: float32 [512], replicated
- w_qa: bfloat16 [7168, 1536], replicated
- w_kva: bfloat16 [7168, 576], replicated
- w_qb: bfloat16 [1536, 12288], P(None, 'tp')
- w_kvb: bfloat16 [512, 16384], P(None, 'tp')
- w_out: bfloat16 [8192, 7168], P('tp')
Outputs:
- output 1: bfloat16 [64, 512, 7168], P('dp')
- output 2: float32 [64], replicated
- output 3: bfloat16 [1536, 12288], P(None, 'tp')
- output 4: bfloat16 [512, 16384], P(None, 'tp')
All inputs are finite; a program needn't handle non-finite values.
Results may differ from the reference program's by a relative error of at most 0.00730254.
Values sent between devices are 32-bit elements.
A program may use at most 1 GiB of HBM per device.

```python
import math
import jax
import jax.numpy as jnp
from jax import lax

B_ALL = 64
SEQ_LEN = 512
D = 7168
HEADS = 64
Q_LORA = 1536
KV_LORA = 512
NOPE_DIM = 128
ROPE_DIM = 64
V_DIM = 128
CLIP_TAU = 100

QK_DIM = NOPE_DIM + ROPE_DIM
NORM_EPS = 1e-6
ROPE_BASE = 50000.0
MSCALE_SQ = (0.1 * math.log(32.0) + 1.0) ** 2
LOGIT_SCALE = QK_DIM ** -0.5 * MSCALE_SQ


def rms_norm(tensor, gain_vec):
    return tensor * lax.rsqrt(jnp.mean(tensor * tensor, axis=-1, keepdims=True) + NORM_EPS) * gain_vec


def rotate(tensor, cos_table, sin_table):
    half_dim = ROPE_DIM // 2
    first_half = tensor[..., :half_dim]
    second_half = tensor[..., half_dim:]
    return jnp.concatenate([first_half * cos_table - second_half * sin_table, first_half * sin_table + second_half * cos_table], axis=-1)


def column_gains(first_gain, first_dim, second_gain, second_dim):
    return jnp.concatenate([jnp.broadcast_to(first_gain[:, None], (HEADS, first_dim)), jnp.broadcast_to(second_gain[:, None], (HEADS, second_dim))], axis=1).reshape(-1)


def setup_inputs(seed: int = 0) -> dict:
    key_list = jax.random.split(jax.random.key(seed), 14)
    common = jax.random.normal(key_list[0], (B_ALL, 1, D), jnp.float32)
    noise_part = jax.random.normal(key_list[1], (B_ALL, SEQ_LEN, D), jnp.float32)
    free_draw = jax.random.randint(key_list[2], (B_ALL,), 0, 64)
    free_pick = jax.random.randint(key_list[3], (), 0, B_ALL)
    independent = (free_draw == 0) | (jnp.arange(B_ALL) == free_pick)
    share_w = jnp.where(independent, 0.0, 0.9)[:, None, None]
    hidden = (share_w * common + jnp.sqrt(1.0 - share_w * share_w) * noise_part).astype(jnp.bfloat16)
    gain_in = 1.0 + 0.2 * jax.random.normal(key_list[4], (D,), jnp.float32)
    gain_q = 1.0 + 0.2 * jax.random.normal(key_list[5], (Q_LORA,), jnp.float32)
    gain_kv = 1.0 + 0.2 * jax.random.normal(key_list[6], (KV_LORA,), jnp.float32)
    w_qa = (jax.random.normal(key_list[7], (D, Q_LORA), jnp.float32) * D ** -0.5).astype(jnp.bfloat16)
    w_kva = (jax.random.normal(key_list[8], (D, KV_LORA + ROPE_DIM), jnp.float32) * D ** -0.5).astype(jnp.bfloat16)
    target = CLIP_TAU / (MSCALE_SQ * math.sqrt(2.0 * math.log(0.5 * SEQ_LEN * SEQ_LEN)))
    head_scale = jnp.exp(jax.random.uniform(key_list[9], (HEADS,), jnp.float32, math.log(0.5), math.log(2.5))) * target
    w_qb = (jax.random.normal(key_list[10], (Q_LORA, HEADS, QK_DIM), jnp.float32) * head_scale[None, :, None] * Q_LORA ** -0.5).reshape(Q_LORA, HEADS * QK_DIM).astype(jnp.bfloat16)
    w_kvb = (jax.random.normal(key_list[11], (KV_LORA, HEADS * (NOPE_DIM + V_DIM)), jnp.float32) * KV_LORA ** -0.5).astype(jnp.bfloat16)
    w_out = (jax.random.normal(key_list[12], (HEADS * V_DIM, D), jnp.float32) * (HEADS * V_DIM) ** -0.5).astype(jnp.bfloat16)
    return {'hidden': hidden, 'gain_in': gain_in, 'gain_q': gain_q, 'gain_kv': gain_kv, 'w_qa': w_qa, 'w_kva': w_kva, 'w_qb': w_qb, 'w_kvb': w_kvb, 'w_out': w_out}


def reference(hidden, gain_in, gain_q, gain_kv, w_qa, w_kva, w_qb, w_kvb, w_out):
    positions = jnp.arange(SEQ_LEN, dtype=jnp.float32)
    inv_freq = ROPE_BASE ** (-2.0 * jnp.arange(ROPE_DIM // 2, dtype=jnp.float32) / ROPE_DIM)
    angles = positions[:, None] * inv_freq[None, :]
    cos_table = jnp.cos(angles)
    sin_table = jnp.sin(angles)
    causal = jnp.arange(SEQ_LEN)[:, None] >= jnp.arange(SEQ_LEN)[None, :]

    def per_sequence(tokens):
        normed = rms_norm(tokens.astype(jnp.float32), gain_in).astype(jnp.bfloat16)
        q_lat = rms_norm(jnp.dot(normed, w_qa, preferred_element_type=jnp.float32), gain_q).astype(jnp.bfloat16)
        kv_lat = jnp.dot(normed, w_kva, preferred_element_type=jnp.float32)
        latent = rms_norm(kv_lat[:, :KV_LORA], gain_kv).astype(jnp.bfloat16)
        k_rot = rotate(kv_lat[:, KV_LORA:], cos_table, sin_table).astype(jnp.bfloat16)
        q_full = jnp.dot(q_lat, w_qb, preferred_element_type=jnp.float32).reshape(SEQ_LEN, HEADS, QK_DIM)
        q_nope = q_full[..., :NOPE_DIM].astype(jnp.bfloat16)
        q_rot = rotate(q_full[..., NOPE_DIM:], cos_table[:, None, :], sin_table[:, None, :]).astype(jnp.bfloat16)
        kv_full = jnp.dot(latent, w_kvb, preferred_element_type=jnp.float32).astype(jnp.bfloat16).reshape(SEQ_LEN, HEADS, NOPE_DIM + V_DIM)
        k_nope = kv_full[..., :NOPE_DIM].astype(jnp.float32)
        values = kv_full[..., NOPE_DIM:].astype(jnp.float32)
        logits = jnp.einsum('qhd,khd->hqk', q_nope.astype(jnp.float32), k_nope) + jnp.einsum('qhd,kd->hqk', q_rot.astype(jnp.float32), k_rot.astype(jnp.float32))
        logits = jnp.where(causal[None], logits * LOGIT_SCALE, -jnp.inf)
        attn_prob = jax.nn.softmax(logits, axis=-1).astype(jnp.bfloat16)
        attn_out = jnp.einsum('hqk,khd->qhd', attn_prob.astype(jnp.float32), values).astype(jnp.bfloat16).reshape(SEQ_LEN, HEADS * V_DIM)
        update = jnp.dot(attn_out, w_out, preferred_element_type=jnp.float32)
        return (tokens.astype(jnp.float32) + update).astype(jnp.bfloat16), jnp.max(logits, axis=(1, 2))

    out_hidden, seq_max = lax.map(per_sequence, hidden)
    logit_max = jnp.max(seq_max, axis=0)
    clip_gain = CLIP_TAU / jnp.maximum(CLIP_TAU, logit_max)
    root_gain = jnp.sqrt(clip_gain)
    new_qb = (w_qb.astype(jnp.float32) * column_gains(root_gain, NOPE_DIM, clip_gain, ROPE_DIM)[None, :]).astype(jnp.bfloat16)
    new_kvb = (w_kvb.astype(jnp.float32) * column_gains(root_gain, NOPE_DIM, jnp.ones_like(clip_gain), V_DIM)[None, :]).astype(jnp.bfloat16)
    return out_hidden, logit_max, new_qb, new_kvb
```

```python
import functools
import math

import jax
import jax.numpy as jnp
from jax import lax
from jax.experimental import pallas as pl
from jax.experimental.pallas import tpu as pltpu
from jax.sharding import PartitionSpec as P

NORM_EPS = 1e-6
ROPE_BASE = 50000.0
MSCALE_SQ = (0.1 * math.log(32.0) + 1.0) ** 2
CLIP_TAU = 100.0
LOG2E = math.log2(math.e)

SEQ = 512
NOPE = 128
ROPE = 64
VDIM = 128
LOGIT_SCALE = (NOPE + ROPE) ** -0.5 * MSCALE_SQ
GROUP = 4
HALF = SEQ // 2
BM = 512
BN = 512
BF16 = jnp.bfloat16
F32 = jnp.float32


def rms_norm(tensor, gain_vec):
    return tensor * lax.rsqrt(jnp.mean(tensor * tensor, axis=-1, keepdims=True) + NORM_EPS) * gain_vec


def rope_tables(rope_dim):
    inv_freq = ROPE_BASE ** (-2.0 * jnp.arange(rope_dim // 2, dtype=F32) / rope_dim)
    angles = jnp.arange(SEQ).astype(F32)[:, None] * inv_freq[None, :]
    return jnp.cos(angles), jnp.sin(angles)


def rotate(tensor, cos_table, sin_table):
    half_dim = tensor.shape[-1] // 2
    first_half = tensor[..., :half_dim]
    second_half = tensor[..., half_dim:]
    return jnp.concatenate([first_half * cos_table - second_half * sin_table, first_half * sin_table + second_half * cos_table], axis=-1)


def dot(a, b):
    return jnp.dot(a, b, preferred_element_type=F32)


def dot_nt(a, b):
    return lax.dot_general(a, b, (((1,), (1,)), ((), ())), preferred_element_type=F32)


def whole(array):
    return pl.BlockSpec(array.shape, lambda *_: (0,) * array.ndim, pipeline_mode=pl.Buffered(1))


def attn_kernel(n_seq, cq_ref, c_ref, kre_ref, kro_ref, wq_ref, wkv_ref, cos_ref, sin_ref, o_ref, s_ref, qa, kva, qb, kvb, *cast):
    if cast:
        wq, wkv = cast
        wq[...] = wq_ref[...].astype(BF16)
        wkv[...] = wkv_ref[...].astype(BF16)
    else:
        wq, wkv = wq_ref, wkv_ref

    def project(b, q_scr, kv_scr):
        rows = pl.ds(pl.multiple_of(b * SEQ, SEQ), SEQ)
        q = dot(cq_ref[rows, :], wq[...])
        lane = lax.broadcasted_iota(jnp.int32, (SEQ, 128), 1)
        low = lane < ROPE
        first = (lane % ROPE) < ROPE // 2
        for p in range(GROUP // 2):
            at = 384 * p
            t0, t1, t2 = q[:, at:at + 128], q[:, at + 128:at + 256], q[:, at + 256:at + 384]
            nope1 = pltpu.roll(jnp.where(low, t2, t1), 64, 1)
            rope = jnp.where(low, t1, t2)
            swapped = jnp.where(first, pltpu.roll(rope, 96, 1), pltpu.roll(rope, 32, 1))
            rope = rope * cos_ref[...] + swapped * sin_ref[...]
            q_scr[:, at:at + 128] = t0.astype(BF16)
            q_scr[:, at + 128:at + 256] = rope.astype(BF16)
            q_scr[:, at + 256:at + 384] = nope1.astype(BF16)
        kv_scr[...] = dot(c_ref[rows, :], wkv[...]).astype(BF16)

    def attend(b, q_scr, kv_scr, maxima):
        start = pl.multiple_of(b * SEQ, SEQ)
        rows = pl.ds(start, SEQ)
        keep = lax.broadcasted_iota(jnp.int32, (HALF, HALF), 0) >= lax.broadcasted_iota(jnp.int32, (HALF, HALF), 1)
        factor = LOGIT_SCALE * LOG2E
        new = []
        for h in range(GROUP):
            at = 384 * (h // 2)
            k_nope = kv_scr[:, 256 * h:256 * h + 128]
            v = kv_scr[:, 256 * h + 128:256 * h + 256]
            if h % 2 == 0:
                q = q_scr[:, at:at + 256]
                k = jnp.concatenate([k_nope, kre_ref[rows, :]], axis=1)
            else:
                q = q_scr[:, at + 128:at + 384]
                k = jnp.concatenate([kro_ref[rows, :], k_nope], axis=1)
            left = dot_nt(q, k[:HALF])
            right = dot_nt(q[HALF:], k[HALF:])
            top = jnp.where(keep, left[:HALF], -jnp.inf)
            low_l = left[HALF:]
            low_r = jnp.where(keep, right, -jnp.inf)
            m0 = jnp.max(top, axis=1, keepdims=True)
            m1 = jnp.max(jnp.maximum(low_l, low_r), axis=1, keepdims=True)
            e0 = jnp.exp2((top - m0) * factor)
            e1 = jnp.exp2((low_l - m1) * factor)
            e2 = jnp.exp2((low_r - m1) * factor)
            inv0 = 1.0 / jnp.sum(e0, axis=1, keepdims=True)
            inv1 = 1.0 / jnp.sum(e1 + e2, axis=1, keepdims=True)
            p_left = jnp.concatenate([(e0 * inv0).astype(BF16), (e1 * inv1).astype(BF16)], axis=0)
            o_left = dot(p_left, v[:HALF])
            o_low = o_left[HALF:] + dot((e2 * inv1).astype(BF16), v[HALF:])
            o_ref[pl.ds(start, HALF), 128 * h:128 * h + 128] = o_left[:HALF].astype(BF16)
            o_ref[pl.ds(pl.multiple_of(start + HALF, HALF), HALF), 128 * h:128 * h + 128] = o_low.astype(BF16)
            new.append(jnp.maximum(maxima[h], jnp.max(jnp.maximum(m0, m1).reshape(HALF // 8, 8, 1), axis=0)))
        return tuple(new)

    maxima = tuple(jnp.full((8, 1), -jnp.inf, F32) for _ in range(GROUP))
    project(0, qa, kva)

    def body(i, maxima):
        project(2 * i + 1, qb, kvb)
        maxima = attend(2 * i, qa, kva, maxima)
        project(jnp.minimum(2 * i + 2, n_seq - 1), qa, kva)
        return attend(2 * i + 1, qb, kvb, maxima)

    maxima = lax.fori_loop(0, n_seq // 2, body, maxima)
    s_ref[0] = jnp.concatenate([jnp.broadcast_to(m * LOGIT_SCALE, (8, 128)) for m in maxima], axis=0)


def attend_heads(c_q, c_kv, kr_even, kr_odd, w_q, w_kv, cos, sin, name):
    tokens = c_q.shape[0]
    heads = w_q.shape[1] // (NOPE + ROPE)
    groups = heads // GROUP
    q_cols, kv_cols = GROUP * (NOPE + ROPE), GROUP * (NOPE + VDIM)
    scratch = [pltpu.VMEM((SEQ, q_cols), BF16), pltpu.VMEM((SEQ, kv_cols), BF16)] * 2
    if w_q.dtype != BF16:
        scratch += [pltpu.VMEM((w_q.shape[0], q_cols), BF16), pltpu.VMEM((w_kv.shape[0], kv_cols), BF16)]
    flops = 2 * tokens * heads * (w_q.shape[0] * 192 + w_kv.shape[0] * 256 + SEQ * 256)
    out, top = pl.pallas_call(
        functools.partial(attn_kernel, tokens // SEQ),
        grid=(groups,),
        in_specs=[whole(c_q), whole(c_kv), whole(kr_even), whole(kr_odd), pl.BlockSpec((w_q.shape[0], q_cols), lambda g: (0, g)), pl.BlockSpec((w_kv.shape[0], kv_cols), lambda g: (0, g)), whole(cos), whole(sin)],
        out_specs=[pl.BlockSpec((tokens, GROUP * VDIM), lambda g: (0, g)), pl.BlockSpec((1, 8 * GROUP, 128), lambda g: (g, 0, 0))],
        out_shape=[jax.ShapeDtypeStruct((tokens, heads * VDIM), BF16), jax.ShapeDtypeStruct((groups, 8 * GROUP, 128), F32)],
        scratch_shapes=scratch,
        compiler_params=pltpu.CompilerParams(vmem_limit_bytes=60 * 1024 * 1024),
        cost_estimate=pl.CostEstimate(flops=flops, bytes_accessed=tokens * heads * VDIM * 2, transcendentals=tokens * heads * SEQ),
        name=name,
    )(c_q, c_kv, kr_even, kr_odd, w_q, w_kv, cos, sin)
    return out, jnp.max(top.reshape(heads, 8, 128)[:, :, 0], axis=1)


def out_kernel(o_own_ref, o_far_ref, w_own_ref, w_far_ref, x_ref, *rest):
    y_ref, w_cast = rest[-2:]

    @pl.when(pl.program_id(1) == 0)
    def _():
        w_cast[...] = w_far_ref[...].astype(BF16)

    total = dot(o_own_ref[...], w_own_ref[...]) + dot(o_far_ref[...], w_cast[...])
    y_ref[...] = (x_ref[...].astype(F32) + total).astype(BF16)


def project_out(o_own, o_far, w_own, w_far, hidden, previous, first_col, name):
    tokens, depth = o_own.shape
    cols = w_far.shape[1]
    base = first_col // BN
    extra = [] if previous is None else [previous]
    return pl.pallas_call(
        out_kernel,
        grid=(cols // BN, tokens // BM),
        in_specs=[
            pl.BlockSpec((BM, depth), lambda n, m: (m, 0)),
            pl.BlockSpec((BM, depth), lambda n, m: (m, 0)),
            pl.BlockSpec((depth, BN), lambda n, m: (0, base + n)),
            pl.BlockSpec((depth, BN), lambda n, m: (0, n)),
            pl.BlockSpec((BM, BN), lambda n, m: (m, base + n)),
        ] + [pl.BlockSpec(memory_space=pl.ANY)] * len(extra),
        out_specs=pl.BlockSpec((BM, BN), lambda n, m: (m, base + n)),
        out_shape=jax.ShapeDtypeStruct(hidden.shape, BF16),
        scratch_shapes=[pltpu.VMEM((depth, BN), BF16)],
        input_output_aliases={5: 0} if extra else {},
        compiler_params=pltpu.CompilerParams(vmem_limit_bytes=60 * 1024 * 1024),
        cost_estimate=pl.CostEstimate(flops=4 * tokens * depth * cols, bytes_accessed=tokens * depth * 4, transcendentals=0),
        name=name,
    )(o_own, o_far, w_own, w_far, hidden, *extra)


def column_gains(first_gain, first_dim, second_gain, second_dim):
    num_heads = first_gain.shape[0]
    return jnp.concatenate([jnp.broadcast_to(first_gain[:, None], (num_heads, first_dim)), jnp.broadcast_to(second_gain[:, None], (num_heads, second_dim))], axis=1).reshape(-1)


def rescale(weight, col_gain):
    return (weight.astype(F32) * col_gain[None, :]).astype(BF16)


COLUMN_CHUNKS = (2048, 2048, 2048, 1024)


def solution(mesh):
    tp, dp = mesh.shape['tp'], mesh.shape['dp']
    swap = [(i, (i + 1) % tp) for i in range(tp)]

    def far_piece(weight, first_col, cols):
        rows = weight.shape[0] // dp
        piece = lax.dynamic_slice(weight, (lax.axis_index('dp') * rows, first_col), (rows, cols)).astype(F32)
        return lax.ppermute(piece, 'tp', swap)

    def gather(piece):
        return lax.all_gather(piece, 'dp', axis=0, tiled=True)

    def device_step(hidden, gain_in, gain_q, gain_kv, w_qa, w_kva, w_qb, w_kvb, w_out):
        num_seqs, seq_len, model_dim = hidden.shape
        kv_rank = gain_kv.shape[0]
        tokens = num_seqs * seq_len
        heads = w_out.shape[0] // VDIM
        starts = [sum(COLUMN_CHUNKS[:i]) for i in range(len(COLUMN_CHUNKS))]
        qb_piece = far_piece(w_qb, 0, w_qb.shape[1])
        kvb_piece = far_piece(w_kvb, 0, w_kvb.shape[1])
        out_pieces = [far_piece(w_out, s, c) for s, c in zip(starts, COLUMN_CHUNKS)]

        cos_table, sin_table = rope_tables(ROPE)
        normed = rms_norm(hidden.astype(F32), gain_in).astype(BF16)
        c_q = rms_norm(jnp.einsum('bsd,dr->bsr', normed, w_qa, preferred_element_type=F32), gain_q).astype(BF16)
        kv_lat = jnp.einsum('bsd,dr->bsr', normed, w_kva, preferred_element_type=F32)
        c_kv = rms_norm(kv_lat[..., :kv_rank], gain_kv).astype(BF16)
        k_rot = rotate(kv_lat[..., kv_rank:], cos_table, sin_table).astype(BF16).reshape(tokens, ROPE)
        blank = jnp.zeros_like(k_rot)
        kr_even = jnp.concatenate([k_rot, blank], axis=1)
        kr_odd = jnp.concatenate([blank, k_rot], axis=1)
        cos = jnp.concatenate([cos_table] * 4, axis=1)
        sin = jnp.concatenate([-sin_table, sin_table] * 2, axis=1)
        c_q, qb_piece, kvb_piece = lax.optimization_barrier((c_q, qb_piece, kvb_piece))
        far_qb, far_kvb = gather(qb_piece), gather(kvb_piece)
        shared = (c_q.reshape(tokens, -1), c_kv.reshape(tokens, -1), kr_even, kr_odd)
        o_own, top_own = attend_heads(*shared, w_qb, w_kvb, cos, sin, 'attend_own')
        o_own, *early = lax.optimization_barrier((o_own, *out_pieces[:3]))
        far_out = [gather(piece) for piece in early]
        o_far, top_far = attend_heads(*shared, far_qb, far_kvb, cos, sin, 'attend_far')

        o_far, late = lax.optimization_barrier((o_far, out_pieces[3]))
        far_out.append(gather(late))

        flat = hidden.reshape(tokens, model_dim)
        y = None
        for i, (s, w_far) in enumerate(zip(starts, far_out)):
            y = project_out(o_own, o_far, w_out, w_far, flat, y, s, f'project_out_{i}')

        first = lax.axis_index('tp') * heads
        top = jnp.zeros((tp * heads,), F32)
        top = lax.dynamic_update_slice(top, top_own, (first,))
        top = lax.dynamic_update_slice(top, top_far, (heads - first,))
        logit_max = lax.pmax(top, ('tp', 'dp'))
        own_max = lax.dynamic_slice(logit_max, (first,), (heads,))
        clip_gain = CLIP_TAU / jnp.maximum(CLIP_TAU, own_max)
        root_gain = jnp.sqrt(clip_gain)
        new_qb = rescale(w_qb, column_gains(root_gain, NOPE, clip_gain, ROPE))
        new_kvb = rescale(w_kvb, column_gains(root_gain, NOPE, jnp.ones_like(clip_gain), VDIM))
        return y.reshape(hidden.shape), logit_max, new_qb, new_kvb

    weight_spec = P(None, 'tp')
    return jax.shard_map(device_step, mesh=mesh, in_specs=(P('dp', None, None), P(), P(), P(), P(), P(), weight_spec, weight_spec, P('tp', None)), out_specs=(P('dp', None, None), P(), weight_spec, weight_spec), check_vma=False)
```

```python
import functools
import math

import jax
import jax.numpy as jnp
from jax import lax
from jax.experimental import pallas as pl
from jax.experimental.pallas import tpu as pltpu
from jax.sharding import PartitionSpec as P

NORM_EPS = 1e-6
ROPE_BASE = 50000.0
MSCALE_SQ = (0.1 * math.log(32.0) + 1.0) ** 2
CLIP_TAU = 100.0
LOG2E = math.log2(math.e)

SEQ = 512
NOPE = 128
ROPE = 64
VDIM = 128
LOGIT_SCALE = (NOPE + ROPE) ** -0.5 * MSCALE_SQ
GROUP = 4
HALF = SEQ // 2
BLOCK = 256
BM = 512
BN = 512
BF16 = jnp.bfloat16
F32 = jnp.float32
VMEM_LIMIT = 60 * 1024 * 1024
COLUMN_CHUNKS = (512, 2048, 2048, 1024, 1024, 512)


def rope_tables(rope_dim):
    inv_freq = ROPE_BASE ** (-2.0 * jnp.arange(rope_dim // 2, dtype=F32) / rope_dim)
    angles = jnp.arange(SEQ).astype(F32)[:, None] * inv_freq[None, :]
    cos, sin = jnp.cos(angles), jnp.sin(angles)
    return jnp.concatenate([cos] * 4, axis=1), jnp.concatenate([-sin, sin] * 2, axis=1)


def dot(a, b):
    return jnp.dot(a, b, preferred_element_type=F32)


def dot_nt(a, b):
    return lax.dot_general(a, b, (((1,), (1,)), ((), ())), preferred_element_type=F32)


def whole(array):
    return pl.BlockSpec(array.shape, lambda *_: (0,) * array.ndim, pipeline_mode=pl.Buffered(1))


def rotate_pairs(rope, cos, sin):
    first = (lax.broadcasted_iota(jnp.int32, rope.shape, 1) % ROPE) < ROPE // 2
    swapped = jnp.where(first, pltpu.roll(rope, 128 - ROPE // 2, 1), pltpu.roll(rope, ROPE // 2, 1))
    return rope * cos + swapped * sin


def kv_latent_kernel(n_seqs, tp_ref, x_ref, gain_ref, w_ref, gkv_ref, cos_ref, sin_ref, n_ref, c_ref, kre_ref, kro_ref, buf_a, buf_b, scales):
    i = pl.program_id(0)
    depth = x_ref.shape[1]
    rank = gkv_ref.shape[1]

    def normalise(first, buf):
        for r in range(0, BLOCK, 8):
            total = jnp.zeros((8, 512), F32)
            for k in range(0, depth, 512):
                part = x_ref[first + r:first + r + 8, k:k + 512].astype(F32)
                total += part * part
            scale = lax.rsqrt(jnp.sum(total, axis=1, keepdims=True) * (1.0 / depth) + NORM_EPS)
            scales[first + r:first + r + 8, :] = jnp.broadcast_to(scale, (8, 128))
        for r in range(0, BLOCK, 8):
            scale = scales[first + r:first + r + 8, :1]
            for k in range(0, depth, 512):
                value = (x_ref[first + r:first + r + 8, k:k + 512].astype(F32) * scale * gain_ref[:, k:k + 512]).astype(BF16)
                n_ref[first + r:first + r + 8, k:k + 512] = value
                buf[r:r + 8, k:k + 512] = value

    def project(buf, block, table):
        a1 = dot(buf[...], w_ref[:, :rank])
        a2 = dot(buf[...], w_ref[:, rank:])
        scale = lax.rsqrt(jnp.mean(a1 * a1, axis=1, keepdims=True) + NORM_EPS)
        rows = pl.ds(pl.multiple_of(block * BLOCK, BLOCK), BLOCK)
        c_ref[rows, :] = (a1 * scale * gkv_ref[...]).astype(BF16)
        pair = rotate_pairs(jnp.concatenate([a2, a2], axis=1), cos_ref[table:table + BLOCK, :], sin_ref[table:table + BLOCK, :])
        low = lax.broadcasted_iota(jnp.int32, pair.shape, 1) < ROPE
        kre_ref[rows, :] = jnp.where(low, pair, 0.0).astype(BF16)
        kro_ref[rows, :] = jnp.where(low, 0.0, pair).astype(BF16)

    project(buf_b, jnp.maximum(2 * i - 1, 0), BLOCK)
    normalise(0, buf_a)
    project(buf_a, 2 * i, 0)
    normalise(BLOCK, buf_b)

    @pl.when(i == n_seqs - 1)
    def _():
        project(buf_b, 2 * i + 1, BLOCK)


def kv_latent(tp_index, x, gain_in, w_kva, gain_kv, cos, sin, n_shared, n_seqs):
    depth = x.shape[1]
    rank = gain_kv.shape[1]
    rows = n_seqs * SEQ

    def source(i, tp):
        return (i + jnp.where(i >= n_shared, tp[0], 0), 0)

    def kept(cols):
        return pl.BlockSpec((rows, cols), lambda i, tp: (0, 0), pipeline_mode=pl.Buffered(1))

    return pl.pallas_call(
        functools.partial(kv_latent_kernel, n_seqs),
        grid_spec=pltpu.PrefetchScalarGridSpec(
            num_scalar_prefetch=1,
            grid=(n_seqs,),
            in_specs=[pl.BlockSpec((SEQ, depth), source), whole(gain_in), whole(w_kva), whole(gain_kv), whole(cos), whole(sin)],
            out_specs=[pl.BlockSpec((SEQ, depth), lambda i, tp: (i, 0)), kept(rank), kept(128), kept(128)],
            scratch_shapes=[pltpu.VMEM((BLOCK, depth), BF16), pltpu.VMEM((BLOCK, depth), BF16), pltpu.VMEM((SEQ, 128), F32)],
        ),
        out_shape=[jax.ShapeDtypeStruct((rows, depth), BF16), jax.ShapeDtypeStruct((rows, rank), BF16), jax.ShapeDtypeStruct((rows, 128), BF16), jax.ShapeDtypeStruct((rows, 128), BF16)],
        compiler_params=pltpu.CompilerParams(vmem_limit_bytes=VMEM_LIMIT),
        cost_estimate=pl.CostEstimate(flops=2 * rows * depth * w_kva.shape[1], bytes_accessed=rows * depth * 4, transcendentals=0),
        name='kv_latent',
    )(tp_index, x, gain_in, w_kva, gain_kv, cos, sin)


def q_latent_kernel(n_blocks, n_ref, w_ref, gq_ref, c_ref, raw):
    i = pl.program_id(0)

    def project():
        raw[i % 2] = dot(n_ref[...], w_ref[...])

    def finish():
        value = raw[(i + 1) % 2]
        scale = lax.rsqrt(jnp.mean(value * value, axis=1, keepdims=True) + NORM_EPS)
        c_ref[...] = (value * scale * gq_ref[...]).astype(BF16)

    @pl.when(i == 0)
    def _():
        project()

    @pl.when((i > 0) & (i < n_blocks))
    def _():
        finish()
        project()

    @pl.when(i == n_blocks)
    def _():
        finish()


def q_latent(normed, w_qa, gain_q):
    rows, depth = normed.shape
    rank = w_qa.shape[1]
    n_blocks = rows // BLOCK
    return pl.pallas_call(
        functools.partial(q_latent_kernel, n_blocks),
        grid=(n_blocks + 1,),
        in_specs=[pl.BlockSpec((BLOCK, depth), lambda i: (jnp.minimum(i, n_blocks - 1), 0)), whole(w_qa), whole(gain_q)],
        out_specs=pl.BlockSpec((BLOCK, rank), lambda i: (jnp.maximum(i - 1, 0), 0)),
        out_shape=jax.ShapeDtypeStruct((rows, rank), BF16),
        scratch_shapes=[pltpu.VMEM((2, BLOCK, rank), F32)],
        compiler_params=pltpu.CompilerParams(vmem_limit_bytes=VMEM_LIMIT),
        cost_estimate=pl.CostEstimate(flops=2 * rows * depth * rank, bytes_accessed=rows * depth * 2, transcendentals=0),
        name='q_latent',
    )(normed, w_qa, gain_q)


def attn_kernel(n_seq, cq_ref, c_ref, kre_ref, kro_ref, wq_ref, wkv_ref, cos_ref, sin_ref, o_ref, s_ref, qa, kva, qb, kvb, *cast):
    if cast:
        wq, wkv = cast
        wq[...] = wq_ref[...].astype(BF16)
        wkv[...] = wkv_ref[...].astype(BF16)
    else:
        wq, wkv = wq_ref, wkv_ref

    def projections(b, q_scr, kv_scr):
        rows = pl.ds(pl.multiple_of(b * SEQ, SEQ), SEQ)

        def even_nope():
            q = dot(cq_ref[rows, :], jnp.concatenate([wq[:, 0:128], wq[:, 384:512]], axis=1)).astype(BF16)
            q_scr[:, 0:256] = q

        def odd_and_rope(at):
            q = dot(cq_ref[rows, :], wq[:, at + 128:at + 384])
            t1, t2 = q[:, :128], q[:, 128:]
            low = lax.broadcasted_iota(jnp.int32, t1.shape, 1) < ROPE
            rope = rotate_pairs(jnp.where(low, t1, t2), cos_ref[...], sin_ref[...])
            nope = pltpu.roll(jnp.where(low, t2, t1), 64, 1)
            first_col = 256 + at // 384 * 256
            q_scr[:, first_col:first_col + 256] = jnp.concatenate([rope, nope], axis=1).astype(BF16)

        def keys_values(heads):
            for h in heads:
                kv_scr[:, 256 * h:256 * h + 256] = dot(c_ref[rows, :], wkv[:, 256 * h:256 * h + 256]).astype(BF16)

        return [even_nope, lambda: odd_and_rope(0), lambda: odd_and_rope(384), lambda: keys_values((0, 1)), lambda: keys_values((2, 3))]

    def attention(b, q_scr, kv_scr):
        start = pl.multiple_of(b * SEQ, SEQ)
        rows = pl.ds(start, SEQ)
        keep = lax.broadcasted_iota(jnp.int32, (HALF, HALF), 0) >= lax.broadcasted_iota(jnp.int32, (HALF, HALF), 1)
        factor = LOGIT_SCALE * LOG2E

        def logits(h):
            at = 256 + 256 * (h // 2)
            k_nope = kv_scr[:, 256 * h:256 * h + 128]
            if h % 2 == 0:
                q = jnp.concatenate([q_scr[:, 64 * h:64 * h + 128], q_scr[:, at:at + 128]], axis=1)
                k = jnp.concatenate([k_nope, kre_ref[rows, :]], axis=1)
            else:
                q = q_scr[:, at:at + 256]
                k = jnp.concatenate([kro_ref[rows, :], k_nope], axis=1)
            return dot_nt(q, k[:HALF]), dot_nt(q[HALF:], k[HALF:])

        def softmax(left, right):
            top = jnp.where(keep, left[:HALF], -jnp.inf)
            low_l = left[HALF:]
            low_r = jnp.where(keep, right, -jnp.inf)
            m0 = jnp.max(top, axis=1, keepdims=True)
            e0 = jnp.exp2((top - m0) * factor)
            p0 = (e0 * (1.0 / jnp.sum(e0, axis=1, keepdims=True))).astype(BF16)
            m1 = jnp.max(jnp.maximum(low_l, low_r), axis=1, keepdims=True)
            e1 = jnp.exp2((low_l - m1) * factor)
            e2 = jnp.exp2((low_r - m1) * factor)
            inv = 1.0 / jnp.sum(e1 + e2, axis=1, keepdims=True)
            biggest = jnp.max(jnp.maximum(m0, m1).reshape(HALF // 8, 8, 1), axis=0)
            return jnp.concatenate([p0, (e1 * inv).astype(BF16)], axis=0), (e2 * inv).astype(BF16), biggest

        def values(h, p_left, p_right, _):
            v = kv_scr[:, 256 * h + 128:256 * h + 256]
            o_left = dot(p_left, v[:HALF])
            return o_left[:HALF], o_left[HALF:] + dot(p_right, v[HALF:])

        def store(h, even, odd):
            cols = slice(128 * h, 128 * h + 256)
            o_ref[pl.ds(start, HALF), cols] = jnp.concatenate([even[0], odd[0]], axis=1).astype(BF16)
            o_ref[pl.ds(pl.multiple_of(start + HALF, HALF), HALF), cols] = jnp.concatenate([even[1], odd[1]], axis=1).astype(BF16)

        return logits, softmax, values, store

    def step(b, held, nxt, spare, maxima):
        logits, softmax, values, store = attention(b, *held)
        parts = [lambda: None] * 5 if spare is None else projections(nxt, *spare)
        l0 = logits(0)
        parts[0]()
        l1 = logits(1)
        p0 = softmax(*l0)
        parts[1]()
        o0 = values(0, *p0)
        l2 = logits(2)
        p1 = softmax(*l1)
        parts[2]()
        store(0, o0, values(1, *p1))
        l3 = logits(3)
        p2 = softmax(*l2)
        parts[3]()
        o2 = values(2, *p2)
        p3 = softmax(*l3)
        parts[4]()
        store(2, o2, values(3, *p3))
        return tuple(jnp.maximum(m, p[2]) for m, p in zip(maxima, (p0, p1, p2, p3)))

    slot_a, slot_b = (qa, kva), (qb, kvb)
    maxima = tuple(jnp.full((8, 1), -jnp.inf, F32) for _ in range(GROUP))
    for part in projections(0, *slot_a):
        part()

    def body(i, maxima):
        maxima = step(2 * i, slot_a, 2 * i + 1, slot_b, maxima)
        return step(2 * i + 1, slot_b, jnp.minimum(2 * i + 2, n_seq - 1), slot_a, maxima)

    maxima = lax.fori_loop(0, n_seq // 2, body, maxima)
    if n_seq % 2:
        maxima = step(n_seq - 1, slot_a, None, None, maxima)
    s_ref[0] = jnp.concatenate([jnp.broadcast_to(m * LOGIT_SCALE, (8, 128)) for m in maxima], axis=0)


def attend_heads(c_q, c_kv, kr_even, kr_odd, w_q, w_kv, cos, sin, name):
    tokens = c_q.shape[0]
    heads = w_q.shape[1] // (NOPE + ROPE)
    groups = heads // GROUP
    q_cols, kv_cols = GROUP * (NOPE + ROPE), GROUP * (NOPE + VDIM)
    scratch = [pltpu.VMEM((SEQ, q_cols), BF16), pltpu.VMEM((SEQ, kv_cols), BF16)] * 2
    if w_q.dtype != BF16:
        scratch += [pltpu.VMEM((w_q.shape[0], q_cols), BF16), pltpu.VMEM((w_kv.shape[0], kv_cols), BF16)]
    flops = 2 * tokens * heads * (w_q.shape[0] * 192 + w_kv.shape[0] * 256 + SEQ * 256)
    out, top = pl.pallas_call(
        functools.partial(attn_kernel, tokens // SEQ),
        grid=(groups,),
        in_specs=[whole(c_q), whole(c_kv), whole(kr_even), whole(kr_odd), pl.BlockSpec((w_q.shape[0], q_cols), lambda g: (0, g)), pl.BlockSpec((w_kv.shape[0], kv_cols), lambda g: (0, g)), whole(cos), whole(sin)],
        out_specs=[pl.BlockSpec((tokens, GROUP * VDIM), lambda g: (0, g)), pl.BlockSpec((1, 8 * GROUP, 128), lambda g: (g, 0, 0))],
        out_shape=[jax.ShapeDtypeStruct((tokens, heads * VDIM), BF16), jax.ShapeDtypeStruct((groups, 8 * GROUP, 128), F32)],
        scratch_shapes=scratch,
        compiler_params=pltpu.CompilerParams(vmem_limit_bytes=VMEM_LIMIT),
        cost_estimate=pl.CostEstimate(flops=flops, bytes_accessed=tokens * heads * VDIM * 2, transcendentals=tokens * heads * SEQ),
        name=name,
    )(c_q, c_kv, kr_even, kr_odd, w_q, w_kv, cos, sin)
    return out, jnp.max(top.reshape(heads, 8, 128)[:, :, 0], axis=1)


def out_kernel(n_shared, tp_ref, o_own_ref, o_far_ref, w_own_ref, w_far_ref, x_ref, *rest):
    y_ref, send_ref, w_cast = rest[-3:]

    @pl.when(pl.program_id(1) == 0)
    def _():
        w_cast[...] = w_far_ref[...].astype(BF16)

    total = dot(o_own_ref[...], w_own_ref[...]) + dot(o_far_ref[...], w_cast[...])
    y_ref[...] = (x_ref[...].astype(F32) + total).astype(BF16)

    @pl.when(pl.program_id(1) >= n_shared)
    def _():
        send_ref[...] = total


def project_out(tp_index, o_own, o_far, w_own, w_far, hidden, previous, first_col, n_shared, name):
    rows, depth = o_own.shape
    cols = w_far.shape[1]
    base = first_col // BN
    extra = [] if previous is None else [previous]

    def place(n, m, tp):
        return (m + jnp.where(m >= n_shared, tp[0], 0), base + n)

    return pl.pallas_call(
        functools.partial(out_kernel, n_shared),
        grid_spec=pltpu.PrefetchScalarGridSpec(
            num_scalar_prefetch=1,
            grid=(cols // BN, rows // BM),
            in_specs=[
                pl.BlockSpec((BM, depth), lambda n, m, tp: (m, 0)),
                pl.BlockSpec((BM, depth), lambda n, m, tp: (m, 0)),
                pl.BlockSpec((depth, BN), lambda n, m, tp: (0, base + n)),
                pl.BlockSpec((depth, BN), lambda n, m, tp: (0, n)),
                pl.BlockSpec((BM, BN), place),
            ] + [pl.BlockSpec(memory_space=pl.ANY)] * len(extra),
            out_specs=[pl.BlockSpec((BM, BN), place), pl.BlockSpec((BM, BN), lambda n, m, tp: (0, n))],
            scratch_shapes=[pltpu.VMEM((depth, BN), BF16)],
        ),
        out_shape=[jax.ShapeDtypeStruct(hidden.shape, BF16), jax.ShapeDtypeStruct((BM, cols), F32)],
        input_output_aliases={6: 0} if extra else {},
        compiler_params=pltpu.CompilerParams(vmem_limit_bytes=VMEM_LIMIT),
        cost_estimate=pl.CostEstimate(flops=4 * rows * depth * cols, bytes_accessed=rows * depth * 4, transcendentals=0),
        name=name,
    )(tp_index, o_own, o_far, w_own, w_far, hidden, *extra)


def column_gains(first_gain, first_dim, second_gain, second_dim):
    num_heads = first_gain.shape[0]
    return jnp.concatenate([jnp.broadcast_to(first_gain[:, None], (num_heads, first_dim)), jnp.broadcast_to(second_gain[:, None], (num_heads, second_dim))], axis=1).reshape(-1)


def rescale(weight, col_gain):
    return (weight.astype(F32) * col_gain[None, :]).astype(BF16)


def solution(mesh):
    tp, dp = mesh.shape['tp'], mesh.shape['dp']
    swap = [(i, (i + 1) % tp) for i in range(tp)]

    def far_piece(weight, first_col, cols):
        rows = weight.shape[0] // dp
        piece = lax.dynamic_slice(weight, (lax.axis_index('dp') * rows, first_col), (rows, cols)).astype(F32)
        return lax.ppermute(piece, 'tp', swap)

    def gather(piece):
        return lax.all_gather(piece, 'dp', axis=0, tiled=True)

    def device_step(hidden, gain_in, gain_q, gain_kv, w_qa, w_kva, w_qb, w_kvb, w_out):
        num_seqs, seq_len, model_dim = hidden.shape
        heads = w_out.shape[0] // VDIM
        n_shared = num_seqs - tp
        tp_at = lax.axis_index('tp')
        tp_index = jnp.full((1,), tp_at, jnp.int32)
        flat = hidden.reshape(num_seqs * seq_len, model_dim)
        starts = [sum(COLUMN_CHUNKS[:i]) for i in range(len(COLUMN_CHUNKS))]

        kvb_piece = far_piece(w_kvb, 0, w_kvb.shape[1])
        cos, sin = rope_tables(ROPE)
        normed, c_kv, kr_even, kr_odd = kv_latent(tp_index, flat, gain_in[None], w_kva, gain_kv[None], cos, sin, n_shared, n_shared + 1)
        out_pieces = [far_piece(w_out, starts[0], COLUMN_CHUNKS[0])]
        qb_piece = far_piece(w_qb, 0, w_qb.shape[1])
        normed, kvb_piece, first = lax.optimization_barrier((normed, kvb_piece, out_pieces[0]))
        far_kvb = gather(kvb_piece)
        far_out = [gather(first)]
        c_q = q_latent(normed, w_qa, gain_q[None])
        out_pieces += [far_piece(w_out, s, c) for s, c in zip(starts[1:], COLUMN_CHUNKS[1:])]
        c_q, qb_piece = lax.optimization_barrier((c_q, qb_piece))
        far_qb = gather(qb_piece)
        latents = (c_q, c_kv, kr_even, kr_odd)
        o_own, top_own = attend_heads(*latents, w_qb, w_kvb, cos, sin, 'attend_own')
        o_own, *ready = lax.optimization_barrier((o_own, *out_pieces[1:4]))
        far_out += [gather(piece) for piece in ready]
        o_far, top_far = attend_heads(*latents, far_qb, far_kvb, cos, sin, 'attend_far')
        o_far, *ready = lax.optimization_barrier((o_far, *out_pieces[4:]))
        far_out += [gather(piece) for piece in ready]

        head_at = tp_at * heads
        top = jnp.zeros((tp * heads,), F32)
        top = lax.dynamic_update_slice(top, top_own, (head_at,))
        top = lax.dynamic_update_slice(top, top_far, (heads - head_at,))
        hops = [('tp', swap)] + [('dp', [(i, i ^ (1 << bit)) for i in range(dp)]) for bit in range(dp.bit_length() - 1)]

        other_row = (num_seqs - 1 - tp_at) * seq_len

        def receive(y, part, first_col):
            cols = part.shape[1]
            rows = lax.dynamic_slice(flat, (other_row, first_col), (seq_len, cols)).astype(F32)
            return lax.dynamic_update_slice(y, (rows + part).astype(BF16), (other_row, first_col))

        y = None
        arriving = []
        for i, (s, w_far) in enumerate(zip(starts, far_out)):
            if i < len(hops):
                hopped = lax.ppermute(top, *hops[i])
            y, part = project_out(tp_index, o_own, o_far, w_out, w_far, flat, y, s, n_shared, f'project_out_{i}')
            if i < len(hops):
                y, top, hopped = lax.optimization_barrier((y, top, hopped))
                top = jnp.maximum(top, hopped)
            if i > 1:
                y = receive(y, *arriving.pop(0))
            arriving.append((lax.ppermute(part, 'tp', swap), s))

        logit_max = top
        own_max = lax.dynamic_slice(logit_max, (head_at,), (heads,))
        clip_gain = CLIP_TAU / jnp.maximum(CLIP_TAU, own_max)
        root_gain = jnp.sqrt(clip_gain)
        new_qb = rescale(w_qb, column_gains(root_gain, NOPE, clip_gain, ROPE))
        new_kvb = rescale(w_kvb, column_gains(root_gain, NOPE, jnp.ones_like(clip_gain), VDIM))
        for part, s in arriving:
            y = receive(y, part, s)
        return y.reshape(hidden.shape), logit_max, new_qb, new_kvb

    weight_spec = P(None, 'tp')
    return jax.shard_map(device_step, mesh=mesh, in_specs=(P('dp', None, None), P(), P(), P(), P(), P(), weight_spec, weight_spec, P('tp', None)), out_specs=(P('dp', None, None), P(), weight_spec, weight_spec), check_vma=False)
```

```python
import functools
import math

import jax
import jax.numpy as jnp
from jax import lax
from jax.experimental import pallas as pl
from jax.experimental.pallas import tpu as pltpu
from jax.sharding import PartitionSpec as P


NORM_EPS = 1e-6
ROPE_BASE = 50000.0
MSCALE_SQ = (0.1 * math.log(32.0) + 1.0) ** 2
CLIP_TAU = 100.0
LOG2E = math.log2(math.e)

SEQ = 512
NOPE = 128
ROPE = 64
VDIM = 128
LOGIT_SCALE = (NOPE + ROPE) ** -0.5 * MSCALE_SQ
GROUP = 4
HALF = SEQ // 2
BLOCK = 256
BM = 896
BN = 256
BF16 = jnp.bfloat16
F32 = jnp.float32
VMEM_LIMIT = 60 * 1024 * 1024
COLUMN_CHUNKS = (2048, 1536, 1280, 1280, 512, 512)


def rope_tables(rope_dim):
    inv_freq = ROPE_BASE ** (-2.0 * jnp.arange(rope_dim // 2, dtype=F32) / rope_dim)
    angles = jnp.arange(SEQ).astype(F32)[:, None] * inv_freq[None, :]
    cos, sin = jnp.cos(angles), jnp.sin(angles)
    return jnp.concatenate([cos] * 4, axis=1), jnp.concatenate([-sin, sin] * 2, axis=1)


def dot(a, b):
    return jnp.dot(a, b, preferred_element_type=F32)


def dot_nt(a, b):
    return lax.dot_general(a, b, (((1,), (1,)), ((), ())), preferred_element_type=F32)


def whole(array):
    return pl.BlockSpec(array.shape, lambda *_: (0,) * array.ndim, pipeline_mode=pl.Buffered(1))


def rotate_pairs(rope, cos, sin):
    first = (lax.broadcasted_iota(jnp.int32, rope.shape, 1) % ROPE) < ROPE // 2
    swapped = jnp.where(first, pltpu.roll(rope, 128 - ROPE // 2, 1), pltpu.roll(rope, ROPE // 2, 1))
    return rope * cos + swapped * sin


def kv_latent_kernel(n_seqs, tp_ref, x_ref, gain_ref, w_ref, gkv_ref, cos_ref, sin_ref, n_ref, c_ref, kre_ref, kro_ref, buf_a, buf_b, scales):
    i = pl.program_id(0)
    depth = x_ref.shape[1]
    rank = gkv_ref.shape[1]

    def normalise(first, buf):
        for r in range(0, BLOCK, 8):
            total = jnp.zeros((8, 512), F32)
            for k in range(0, depth, 512):
                part = x_ref[first + r:first + r + 8, k:k + 512].astype(F32)
                total += part * part
            scale = lax.rsqrt(jnp.sum(total, axis=1, keepdims=True) * (1.0 / depth) + NORM_EPS)
            scales[first + r:first + r + 8, :] = jnp.broadcast_to(scale, (8, 128))
        for r in range(0, BLOCK, 8):
            scale = scales[first + r:first + r + 8, :1]
            for k in range(0, depth, 512):
                value = (x_ref[first + r:first + r + 8, k:k + 512].astype(F32) * scale * gain_ref[:, k:k + 512]).astype(BF16)
                n_ref[first + r:first + r + 8, k:k + 512] = value
                buf[r:r + 8, k:k + 512] = value

    def project(buf, block, table):
        a1 = dot_nt(buf[...], w_ref[:rank, :])
        a2 = dot_nt(buf[...], w_ref[rank:, :])
        scale = lax.rsqrt(jnp.mean(a1 * a1, axis=1, keepdims=True) + NORM_EPS)
        rows = pl.ds(pl.multiple_of(block * BLOCK, BLOCK), BLOCK)
        c_ref[rows, :] = (a1 * scale * gkv_ref[...]).astype(BF16)
        pair = rotate_pairs(jnp.concatenate([a2, a2], axis=1), cos_ref[table:table + BLOCK, :], sin_ref[table:table + BLOCK, :])
        low = lax.broadcasted_iota(jnp.int32, pair.shape, 1) < ROPE
        kre_ref[rows, :] = jnp.where(low, pair, 0.0).astype(BF16)
        kro_ref[rows, :] = jnp.where(low, 0.0, pair).astype(BF16)

    project(buf_b, jnp.maximum(2 * i - 1, 0), BLOCK)
    normalise(0, buf_a)
    project(buf_a, 2 * i, 0)
    normalise(BLOCK, buf_b)

    @pl.when(i == n_seqs - 1)
    def _():
        project(buf_b, 2 * i + 1, BLOCK)


def kv_latent(tp_index, x, gain_in, w_kva, gain_kv, cos, sin, n_seqs):
    depth = x.shape[1]
    rank = gain_kv.shape[1]
    rows = n_seqs * SEQ

    def kept(cols):
        return pl.BlockSpec((rows, cols), lambda i, tp: (0, 0), pipeline_mode=pl.Buffered(1))

    return pl.pallas_call(
        functools.partial(kv_latent_kernel, n_seqs),
        grid_spec=pltpu.PrefetchScalarGridSpec(
            num_scalar_prefetch=1,
            grid=(n_seqs,),
            in_specs=[pl.BlockSpec((SEQ, depth), lambda i, tp: (i + tp[0], 0)), whole(gain_in), whole(w_kva), whole(gain_kv), whole(cos), whole(sin)],
            out_specs=[pl.BlockSpec((SEQ, depth), lambda i, tp: (i, 0)), kept(rank), kept(128), kept(128)],
            scratch_shapes=[pltpu.VMEM((BLOCK, depth), BF16), pltpu.VMEM((BLOCK, depth), BF16), pltpu.VMEM((SEQ, 128), F32)],
        ),
        out_shape=[jax.ShapeDtypeStruct((rows, depth), BF16), jax.ShapeDtypeStruct((rows, rank), BF16), jax.ShapeDtypeStruct((rows, 128), BF16), jax.ShapeDtypeStruct((rows, 128), BF16)],
        compiler_params=pltpu.CompilerParams(vmem_limit_bytes=VMEM_LIMIT),
        cost_estimate=pl.CostEstimate(flops=2 * rows * depth * w_kva.shape[0], bytes_accessed=rows * depth * 4, transcendentals=0),
        name='kv_latent',
    )(tp_index, x, gain_in, w_kva, gain_kv, cos, sin)


def q_latent_kernel(n_blocks, n_ref, w_ref, gq_ref, c_ref, raw):
    i = pl.program_id(0)

    def project():
        raw[i % 2] = dot(n_ref[...], w_ref[...])

    def finish():
        value = raw[(i + 1) % 2]
        scale = lax.rsqrt(jnp.mean(value * value, axis=1, keepdims=True) + NORM_EPS)
        c_ref[...] = (value * scale * gq_ref[...]).astype(BF16)

    @pl.when(i == 0)
    def _():
        project()

    @pl.when((i > 0) & (i < n_blocks))
    def _():
        finish()
        project()

    @pl.when(i == n_blocks)
    def _():
        finish()


def q_latent(normed, w_qa, gain_q):
    rows, depth = normed.shape
    rank = w_qa.shape[1]
    n_blocks = rows // BLOCK
    return pl.pallas_call(
        functools.partial(q_latent_kernel, n_blocks),
        grid=(n_blocks + 1,),
        in_specs=[pl.BlockSpec((BLOCK, depth), lambda i: (jnp.minimum(i, n_blocks - 1), 0)), whole(w_qa), whole(gain_q)],
        out_specs=pl.BlockSpec((BLOCK, rank), lambda i: (jnp.maximum(i - 1, 0), 0)),
        out_shape=jax.ShapeDtypeStruct((rows, rank), BF16),
        scratch_shapes=[pltpu.VMEM((2, BLOCK, rank), F32)],
        compiler_params=pltpu.CompilerParams(vmem_limit_bytes=VMEM_LIMIT),
        cost_estimate=pl.CostEstimate(flops=2 * rows * depth * rank, bytes_accessed=rows * depth * 2, transcendentals=0),
        name='q_latent',
    )(normed, w_qa, gain_q)


def attn_kernel(n_seq, cq_ref, c_ref, kre_ref, kro_ref, wq_ref, wkv_ref, cos_ref, sin_ref, o_ref, s_ref, qa, kva, qb, kvb, *cast):
    if cast:
        wq, wkv = cast
        wq[...] = wq_ref[...].astype(BF16)
        wkv[...] = wkv_ref[...].astype(BF16)
    else:
        wq, wkv = wq_ref, wkv_ref

    def projections(b, q_scr, kv_scr):
        rows = pl.ds(pl.multiple_of(b * SEQ, SEQ), SEQ)

        def even_nope():
            q = dot(cq_ref[rows, :], jnp.concatenate([wq[:, 0:128], wq[:, 384:512]], axis=1)).astype(BF16)
            q_scr[:, 0:256] = q

        def odd_and_rope(at):
            q = dot(cq_ref[rows, :], wq[:, at + 128:at + 384])
            t1, t2 = q[:, :128], q[:, 128:]
            low = lax.broadcasted_iota(jnp.int32, t1.shape, 1) < ROPE
            rope = rotate_pairs(jnp.where(low, t1, t2), cos_ref[...], sin_ref[...])
            nope = pltpu.roll(jnp.where(low, t2, t1), 64, 1)
            first_col = 256 + at // 384 * 256
            q_scr[:, first_col:first_col + 256] = jnp.concatenate([rope, nope], axis=1).astype(BF16)

        def keys_values(heads):
            for h in heads:
                kv_scr[:, 256 * h:256 * h + 256] = dot(c_ref[rows, :], wkv[:, 256 * h:256 * h + 256]).astype(BF16)

        return [even_nope, lambda: odd_and_rope(0), lambda: odd_and_rope(384), lambda: keys_values((0, 1)), lambda: keys_values((2, 3))]

    def attention(b, q_scr, kv_scr):
        start = pl.multiple_of(b * SEQ, SEQ)
        rows = pl.ds(start, SEQ)
        keep = lax.broadcasted_iota(jnp.int32, (HALF, HALF), 0) >= lax.broadcasted_iota(jnp.int32, (HALF, HALF), 1)
        factor = LOGIT_SCALE * LOG2E

        def logits(h):
            at = 256 + 256 * (h // 2)
            k_nope = kv_scr[:, 256 * h:256 * h + 128]
            if h % 2 == 0:
                q = jnp.concatenate([q_scr[:, 64 * h:64 * h + 128], q_scr[:, at:at + 128]], axis=1)
                k = jnp.concatenate([k_nope, kre_ref[rows, :]], axis=1)
            else:
                q = q_scr[:, at:at + 256]
                k = jnp.concatenate([kro_ref[rows, :], k_nope], axis=1)
            return dot_nt(q, k[:HALF]), dot_nt(q[HALF:], k[HALF:])

        def softmax(left, right):
            top = jnp.where(keep, left[:HALF], -jnp.inf)
            low_l = left[HALF:]
            low_r = jnp.where(keep, right, -jnp.inf)
            m0 = jnp.max(top, axis=1, keepdims=True)
            e0 = jnp.exp2((top - m0) * factor)
            p0 = (e0 * (1.0 / jnp.sum(e0, axis=1, keepdims=True))).astype(BF16)
            m1 = jnp.max(jnp.maximum(low_l, low_r), axis=1, keepdims=True)
            e1 = jnp.exp2((low_l - m1) * factor)
            e2 = jnp.exp2((low_r - m1) * factor)
            inv = 1.0 / jnp.sum(e1 + e2, axis=1, keepdims=True)
            biggest = jnp.max(jnp.maximum(m0, m1).reshape(HALF // 8, 8, 1), axis=0)
            return jnp.concatenate([p0, (e1 * inv).astype(BF16)], axis=0), (e2 * inv).astype(BF16), biggest

        def values(h, p_left, p_right, _):
            v = kv_scr[:, 256 * h + 128:256 * h + 256]
            o_left = dot(p_left, v[:HALF])
            return o_left[:HALF], o_left[HALF:] + dot(p_right, v[HALF:])

        def store(h, even, odd):
            cols = slice(128 * h, 128 * h + 256)
            o_ref[pl.ds(start, HALF), cols] = jnp.concatenate([even[0], odd[0]], axis=1).astype(BF16)
            o_ref[pl.ds(pl.multiple_of(start + HALF, HALF), HALF), cols] = jnp.concatenate([even[1], odd[1]], axis=1).astype(BF16)

        return logits, softmax, values, store

    def step(b, held, nxt, spare, maxima):
        logits, softmax, values, store = attention(b, *held)
        parts = [lambda: None] * 5 if spare is None else projections(nxt, *spare)
        l0 = logits(0)
        parts[0]()
        l1 = logits(1)
        p0 = softmax(*l0)
        parts[1]()
        o0 = values(0, *p0)
        l2 = logits(2)
        p1 = softmax(*l1)
        parts[2]()
        store(0, o0, values(1, *p1))
        l3 = logits(3)
        p2 = softmax(*l2)
        parts[3]()
        o2 = values(2, *p2)
        p3 = softmax(*l3)
        parts[4]()
        store(2, o2, values(3, *p3))
        return tuple(jnp.maximum(m, p[2]) for m, p in zip(maxima, (p0, p1, p2, p3)))

    slot_a, slot_b = (qa, kva), (qb, kvb)
    maxima = tuple(jnp.full((8, 1), -jnp.inf, F32) for _ in range(GROUP))
    for part in projections(0, *slot_a):
        part()

    def body(i, maxima):
        maxima = step(2 * i, slot_a, 2 * i + 1, slot_b, maxima)
        return step(2 * i + 1, slot_b, jnp.minimum(2 * i + 2, n_seq - 1), slot_a, maxima)

    maxima = lax.fori_loop(0, n_seq // 2, body, maxima)
    if n_seq % 2:
        maxima = step(n_seq - 1, slot_a, None, None, maxima)
    s_ref[0] = jnp.concatenate([jnp.broadcast_to(m * LOGIT_SCALE, (8, 128)) for m in maxima], axis=0)


def attend_heads(c_q, c_kv, kr_even, kr_odd, w_q, w_kv, cos, sin):
    tokens = c_q.shape[0]
    heads = w_q.shape[1] // (NOPE + ROPE)
    groups = heads // GROUP
    q_cols, kv_cols = GROUP * (NOPE + ROPE), GROUP * (NOPE + VDIM)
    scratch = [pltpu.VMEM((SEQ, q_cols), BF16), pltpu.VMEM((SEQ, kv_cols), BF16)] * 2
    if w_q.dtype != BF16:
        scratch += [pltpu.VMEM((w_q.shape[0], q_cols), BF16), pltpu.VMEM((w_kv.shape[0], kv_cols), BF16)]
    flops = 2 * tokens * heads * (w_q.shape[0] * 192 + w_kv.shape[0] * 256 + SEQ * 256)
    out, top = pl.pallas_call(
        functools.partial(attn_kernel, tokens // SEQ),
        grid=(groups,),
        in_specs=[whole(c_q), whole(c_kv), whole(kr_even), whole(kr_odd), pl.BlockSpec((w_q.shape[0], q_cols), lambda g: (0, g)), pl.BlockSpec((w_kv.shape[0], kv_cols), lambda g: (0, g)), whole(cos), whole(sin)],
        out_specs=[pl.BlockSpec((tokens, GROUP * VDIM), lambda g: (0, g)), pl.BlockSpec((1, 8 * GROUP, 128), lambda g: (g, 0, 0))],
        out_shape=[jax.ShapeDtypeStruct((tokens, heads * VDIM), BF16), jax.ShapeDtypeStruct((groups, 8 * GROUP, 128), F32)],
        scratch_shapes=scratch,
        compiler_params=pltpu.CompilerParams(vmem_limit_bytes=VMEM_LIMIT),
        cost_estimate=pl.CostEstimate(flops=flops, bytes_accessed=tokens * heads * VDIM * 2, transcendentals=tokens * heads * SEQ),
    )(c_q, c_kv, kr_even, kr_odd, w_q, w_kv, cos, sin)
    return out, jnp.max(top.reshape(heads, 8, 128)[:, :, 0], axis=1)


def out_kernel(n_cols, has_prev, tp_ref, o_own, o_far, w_own, w_far, x_hbm, *rest):
    if has_prev:
        y_hbm, send, own_buf, far_buf, wo_buf, wf_buf, x_buf, y_buf, t_buf, o_sem, w_sem, x_sem, y_sem, t_sem = rest[1:]
    else:
        y_hbm, send, own_buf, far_buf, wo_buf, wf_buf, x_buf, y_buf, t_buf, o_sem, w_sem, x_sem, y_sem, t_sem = rest
    first_col, tp_at = tp_ref[1], tp_ref[0]
    n_rows = o_own.shape[0] // BM
    s = pl.program_id(0)
    steps = n_rows * n_cols
    m, n = s // n_cols, s % n_cols
    slot = s % 2

    def o_copies(m):
        rows = pl.ds(pl.multiple_of(m * BM, 128), BM)
        return (pltpu.make_async_copy(o_own.at[rows, :], own_buf.at[m % 2], o_sem.at[0, m % 2]), pltpu.make_async_copy(o_far.at[rows, :], far_buf.at[m % 2], o_sem.at[1, m % 2]))

    def w_copies(s):
        col = (s % n_cols) * BN
        own_cols = pl.ds(pl.multiple_of(first_col + col, BN), BN)
        far_cols = pl.ds(pl.multiple_of(col, BN), BN)
        rows = pl.ds(pl.multiple_of(s // n_cols * BM + tp_at * SEQ, 128), BM)
        k = s % 2
        return (
            pltpu.make_async_copy(w_own.at[:, own_cols], wo_buf.at[k], w_sem.at[0, k]),
            pltpu.make_async_copy(w_far.at[:, far_cols], wf_buf.at[k], w_sem.at[1, k]),
            pltpu.make_async_copy(x_hbm.at[rows, own_cols], x_buf.at[k], x_sem.at[k]),
        )

    def y_copy(s):
        own_cols = pl.ds(pl.multiple_of(first_col + (s % n_cols) * BN, BN), BN)
        rows = pl.ds(pl.multiple_of(s // n_cols * BM + tp_at * SEQ, 128), BM)
        return pltpu.make_async_copy(y_buf.at[s % 2], y_hbm.at[rows, own_cols], y_sem.at[s % 2])

    def t_copy(n):
        inner = pl.multiple_of(tp_at * (BM - SEQ), 128)
        return pltpu.make_async_copy(t_buf.at[n % 2, pl.ds(inner, SEQ), :], send.at[:, pl.ds(pl.multiple_of(n * BN, BN), BN)], t_sem.at[n % 2])

    @pl.when(s == 0)
    def _():
        for copy in w_copies(0) + o_copies(0):
            copy.start()

    @pl.when(s + 1 < steps)
    def _():
        for copy in w_copies(s + 1):
            copy.start()

    @pl.when((n == 0) & (m + 1 < n_rows))
    def _():
        for copy in o_copies(m + 1):
            copy.start()

    @pl.when(n == 0)
    def _():
        for copy in o_copies(m):
            copy.wait()

    @pl.when(s >= 2)
    def _():
        y_copy(s - 2).wait()

    exclusive = m == tp_at * (n_rows - 1)

    @pl.when(exclusive & (n >= 2))
    def _():
        t_copy(n - 2).wait()

    for copy in w_copies(s):
        copy.wait()
    total = dot(own_buf[m % 2], wo_buf[slot]) + dot(far_buf[m % 2], wf_buf[slot].astype(BF16))
    t_buf[n % 2] = total
    y_buf[slot] = (x_buf[slot].astype(F32) + total).astype(BF16)
    y_copy(s).start()

    @pl.when(exclusive)
    def _():
        t_copy(n).start()

    @pl.when(exclusive & (n == n_cols - 1))
    def _():
        for k in range(max(0, n_cols - 2), n_cols):
            t_copy(k).wait()

    @pl.when(s == steps - 1)
    def _():
        y_copy(s - 1).wait()
        y_copy(s).wait()


def project_out(tp_at, o_own, o_far, w_own, w_far, hidden, previous, first_col):
    rows, depth = o_own.shape
    cols = w_far.shape[1]
    n_cols = cols // BN
    extra = [] if previous is None else [previous]
    return pl.pallas_call(
        functools.partial(out_kernel, n_cols, bool(extra)),
        grid_spec=pltpu.PrefetchScalarGridSpec(
            num_scalar_prefetch=1,
            grid=(rows // BM * n_cols,),
            in_specs=[pl.BlockSpec(memory_space=pl.ANY)] * (5 + len(extra)),
            out_specs=[pl.BlockSpec(memory_space=pl.ANY)] * 2,
            scratch_shapes=[
                pltpu.VMEM((2, BM, depth), BF16),
                pltpu.VMEM((2, BM, depth), BF16),
                pltpu.VMEM((2, depth, BN), BF16),
                pltpu.VMEM((2, depth, BN), F32),
                pltpu.VMEM((2, BM, BN), BF16),
                pltpu.VMEM((2, BM, BN), BF16),
                pltpu.VMEM((2, BM, BN), F32),
                pltpu.SemaphoreType.DMA((2, 2)),
                pltpu.SemaphoreType.DMA((2, 2)),
                pltpu.SemaphoreType.DMA((2,)),
                pltpu.SemaphoreType.DMA((2,)),
                pltpu.SemaphoreType.DMA((2,)),
            ],
        ),
        out_shape=[jax.ShapeDtypeStruct(hidden.shape, BF16), jax.ShapeDtypeStruct((SEQ, cols), F32)],
        input_output_aliases={6: 0} if extra else {},
        compiler_params=pltpu.CompilerParams(vmem_limit_bytes=VMEM_LIMIT),
        cost_estimate=pl.CostEstimate(flops=4 * rows * depth * cols, bytes_accessed=rows * depth * 4, transcendentals=0),
    )(jnp.stack([tp_at, jnp.int32(first_col)]), o_own, o_far, w_own, w_far, hidden, *extra)


def column_gains(first_gain, first_dim, second_gain, second_dim):
    num_heads = first_gain.shape[0]
    return jnp.concatenate([jnp.broadcast_to(first_gain[:, None], (num_heads, first_dim)), jnp.broadcast_to(second_gain[:, None], (num_heads, second_dim))], axis=1).reshape(-1)


def rescale(weight, col_gain):
    return (weight.astype(F32) * col_gain[None, :]).astype(BF16)


def solution(mesh):
    tp, dp = mesh.shape['tp'], mesh.shape['dp']
    swap = [(i, (i + 1) % tp) for i in range(tp)]

    def far_piece(weight, first_col, cols):
        rows = weight.shape[0] // dp
        piece = lax.dynamic_slice(weight, (lax.axis_index('dp') * rows, first_col), (rows, cols)).astype(F32)
        return lax.ppermute(piece, 'tp', swap)

    def gather(piece):
        return lax.all_gather(piece, 'dp', axis=0, tiled=True)

    def device_step(hidden, gain_in, gain_q, gain_kv, w_qa, w_kva, w_qb, w_kvb, w_out):
        num_seqs, seq_len, model_dim = hidden.shape
        heads = w_out.shape[0] // VDIM
        tp_at = lax.axis_index('tp').astype(jnp.int32)
        flat = hidden.reshape(num_seqs * seq_len, model_dim)
        starts = [sum(COLUMN_CHUNKS[:i]) for i in range(len(COLUMN_CHUNKS))]

        kvb_piece = far_piece(w_kvb, 0, w_kvb.shape[1])
        qb_piece = far_piece(w_qb, 0, w_qb.shape[1])
        out_pieces = [far_piece(w_out, s, c) for s, c in zip(starts, COLUMN_CHUNKS)]
        cos, sin = rope_tables(ROPE)
        normed, c_kv, kr_even, kr_odd = kv_latent(tp_at[None], flat, gain_in[None], w_kva.T, gain_kv[None], cos, sin, num_seqs - tp + 1)
        normed, kvb_piece = lax.optimization_barrier((normed, kvb_piece))
        far_kvb = gather(kvb_piece)
        c_q = q_latent(normed, w_qa, gain_q[None])
        c_q, qb_piece = lax.optimization_barrier((c_q, qb_piece))
        far_qb = gather(qb_piece)
        latents = (c_q, c_kv, kr_even, kr_odd)
        o_own, top_own = attend_heads(*latents, w_qb, w_kvb, cos, sin)
        o_own, *ready = lax.optimization_barrier((o_own, *out_pieces[:2]))
        far_out = [gather(piece) for piece in ready]
        o_far, top_far = attend_heads(*latents, far_qb, far_kvb, cos, sin)
        o_far, *ready = lax.optimization_barrier((o_far, *out_pieces[2:]))
        far_out += [gather(piece) for piece in ready]

        head_at = tp_at * heads
        top = jnp.zeros((tp * heads,), F32)
        top = lax.dynamic_update_slice(top, top_own, (head_at,))
        top = lax.dynamic_update_slice(top, top_far, (heads - head_at,))
        hops = [('tp', swap)] + [('dp', [(i, i ^ (1 << bit)) for i in range(dp)]) for bit in range(dp.bit_length() - 1)]

        other_row = (1 - tp_at) * (num_seqs - 1) * seq_len

        def receive(y, part, first_col):
            cols = part.shape[1]
            rows = lax.dynamic_slice(flat, (other_row, first_col), (seq_len, cols)).astype(F32)
            return lax.dynamic_update_slice(y, (rows + part).astype(BF16), (other_row, first_col))

        y = None
        arriving = []
        for i, (s, w_far) in enumerate(zip(starts, far_out)):
            if i < len(hops):
                hopped = lax.ppermute(top, *hops[i])
            y, part = project_out(tp_at, o_own, o_far, w_out, w_far, flat, y, s)
            if i < len(hops):
                y, top, hopped = lax.optimization_barrier((y, top, hopped))
                top = jnp.maximum(top, hopped)
            if i > 1:
                y = receive(y, *arriving.pop(0))
            arriving.append((lax.ppermute(part, 'tp', swap), s))

        logit_max = top
        own_max = lax.dynamic_slice(logit_max, (head_at,), (heads,))
        clip_gain = CLIP_TAU / jnp.maximum(CLIP_TAU, own_max)
        root_gain = jnp.sqrt(clip_gain)
        new_qb = rescale(w_qb, column_gains(root_gain, NOPE, clip_gain, ROPE))
        new_kvb = rescale(w_kvb, column_gains(root_gain, NOPE, jnp.ones_like(clip_gain), VDIM))
        for part, s in arriving:
            y = receive(y, part, s)
        return y.reshape(hidden.shape), logit_max, new_qb, new_kvb

    weight_spec = P(None, 'tp')
    return jax.shard_map(device_step, mesh=mesh, in_specs=(P('dp', None, None), P(), P(), P(), P(), P(), weight_spec, weight_spec, P('tp', None)), out_specs=(P('dp', None, None), P(), weight_spec, weight_spec), check_vma=False)
```

```python
import functools
import math

import jax
import jax.numpy as jnp
from jax import lax
from jax.experimental import pallas as pl
from jax.experimental.pallas import tpu as pltpu
from jax.sharding import PartitionSpec as P


NORM_EPS = 1e-6
ROPE_BASE = 50000.0
MSCALE_SQ = (0.1 * math.log(32.0) + 1.0) ** 2
CLIP_TAU = 100.0
LOG2E = math.log2(math.e)

SEQ = 512
NOPE = 128
ROPE = 64
VDIM = 128
LOGIT_SCALE = (NOPE + ROPE) ** -0.5 * MSCALE_SQ
GROUP = 4
HALF = SEQ // 2
BLOCK = 256
BM = 896
BN = 256
BF16 = jnp.bfloat16
F32 = jnp.float32
VMEM_LIMIT = 60 * 1024 * 1024
COLUMN_CHUNKS = (2048, 2048, 1536, 1024, 512)
PIECE = 512


def rope_tables(rope_dim):
    inv_freq = ROPE_BASE ** (-2.0 * jnp.arange(rope_dim // 2, dtype=F32) / rope_dim)
    angles = jnp.arange(SEQ).astype(F32)[:, None] * inv_freq[None, :]
    cos, sin = jnp.cos(angles), jnp.sin(angles)
    return jnp.concatenate([cos] * 4, axis=1), jnp.concatenate([-sin, sin] * 2, axis=1)


def dot(a, b):
    return jnp.dot(a, b, preferred_element_type=F32)


def dot_nt(a, b):
    return lax.dot_general(a, b, (((1,), (1,)), ((), ())), preferred_element_type=F32)


def whole(array):
    return pl.BlockSpec(array.shape, lambda *_: (0,) * array.ndim, pipeline_mode=pl.Buffered(1))


def rotate_pairs(rope, cos, sin):
    first = (lax.broadcasted_iota(jnp.int32, rope.shape, 1) % ROPE) < ROPE // 2
    swapped = jnp.where(first, pltpu.roll(rope, 128 - ROPE // 2, 1), pltpu.roll(rope, ROPE // 2, 1))
    return rope * cos + swapped * sin


def kv_latent_kernel(n_seqs, tp_ref, x_ref, gain_ref, w_ref, gkv_ref, cos_ref, sin_ref, n_ref, c_ref, kre_ref, kro_ref, buf_a, buf_b, scales):
    i = pl.program_id(0)
    depth = x_ref.shape[1]
    rank = gkv_ref.shape[1]

    def normalise(first, buf):
        for r in range(0, BLOCK, 8):
            total = jnp.zeros((8, 512), F32)
            for k in range(0, depth, 512):
                part = x_ref[first + r:first + r + 8, k:k + 512].astype(F32)
                total += part * part
            scale = lax.rsqrt(jnp.sum(total, axis=1, keepdims=True) * (1.0 / depth) + NORM_EPS)
            scales[first + r:first + r + 8, :] = jnp.broadcast_to(scale, (8, 128))
        for r in range(0, BLOCK, 8):
            scale = scales[first + r:first + r + 8, :1]
            for k in range(0, depth, 512):
                value = (x_ref[first + r:first + r + 8, k:k + 512].astype(F32) * scale * gain_ref[:, k:k + 512]).astype(BF16)
                n_ref[first + r:first + r + 8, k:k + 512] = value
                buf[r:r + 8, k:k + 512] = value

    def project(buf, block, table):
        a1 = dot_nt(buf[...], w_ref[:rank, :])
        a2 = dot_nt(buf[...], w_ref[rank:, :])
        scale = lax.rsqrt(jnp.mean(a1 * a1, axis=1, keepdims=True) + NORM_EPS)
        rows = pl.ds(pl.multiple_of(block * BLOCK, BLOCK), BLOCK)
        c_ref[rows, :] = (a1 * scale * gkv_ref[...]).astype(BF16)
        pair = rotate_pairs(jnp.concatenate([a2, a2], axis=1), cos_ref[table:table + BLOCK, :], sin_ref[table:table + BLOCK, :])
        low = lax.broadcasted_iota(jnp.int32, pair.shape, 1) < ROPE
        kre_ref[rows, :] = jnp.where(low, pair, 0.0).astype(BF16)
        kro_ref[rows, :] = jnp.where(low, 0.0, pair).astype(BF16)

    project(buf_b, jnp.maximum(2 * i - 1, 0), BLOCK)
    normalise(0, buf_a)
    project(buf_a, 2 * i, 0)
    normalise(BLOCK, buf_b)

    @pl.when(i == n_seqs - 1)
    def _():
        project(buf_b, 2 * i + 1, BLOCK)


def kv_latent(tp_index, x, gain_in, w_kva, gain_kv, cos, sin, n_seqs):
    depth = x.shape[1]
    rank = gain_kv.shape[1]
    rows = n_seqs * SEQ

    def kept(cols):
        return pl.BlockSpec((rows, cols), lambda i, tp: (0, 0), pipeline_mode=pl.Buffered(1))

    return pl.pallas_call(
        functools.partial(kv_latent_kernel, n_seqs),
        grid_spec=pltpu.PrefetchScalarGridSpec(
            num_scalar_prefetch=1,
            grid=(n_seqs,),
            in_specs=[pl.BlockSpec((SEQ, depth), lambda i, tp: (i + tp[0], 0)), whole(gain_in), whole(w_kva), whole(gain_kv), whole(cos), whole(sin)],
            out_specs=[pl.BlockSpec((SEQ, depth), lambda i, tp: (i, 0)), kept(rank), kept(128), kept(128)],
            scratch_shapes=[pltpu.VMEM((BLOCK, depth), BF16), pltpu.VMEM((BLOCK, depth), BF16), pltpu.VMEM((SEQ, 128), F32)],
        ),
        out_shape=[jax.ShapeDtypeStruct((rows, depth), BF16), jax.ShapeDtypeStruct((rows, rank), BF16), jax.ShapeDtypeStruct((rows, 128), BF16), jax.ShapeDtypeStruct((rows, 128), BF16)],
        compiler_params=pltpu.CompilerParams(vmem_limit_bytes=VMEM_LIMIT),
        cost_estimate=pl.CostEstimate(flops=2 * rows * depth * w_kva.shape[0], bytes_accessed=rows * depth * 4, transcendentals=0),
        name='kv_latent',
    )(tp_index, x, gain_in, w_kva, gain_kv, cos, sin)


def q_latent_kernel(n_blocks, chunks, ids_ref, n_ref, w_ref, gq_ref, wo_ref, c_ref, *rest):
    pieces, raw = rest[:-1], rest[-1]
    i = pl.program_id(0)
    first = 0
    for piece, cols in zip(pieces, chunks):
        @pl.when((i >= first) & (i < first + cols // PIECE))
        def _(piece=piece):
            piece[...] = wo_ref[...].astype(F32)

        first += cols // PIECE

    def project():
        raw[i % 2] = dot(n_ref[...], w_ref[...])

    def finish():
        value = raw[(i + 1) % 2]
        scale = lax.rsqrt(jnp.mean(value * value, axis=1, keepdims=True) + NORM_EPS)
        c_ref[...] = (value * scale * gq_ref[...]).astype(BF16)

    @pl.when(i == 0)
    def _():
        project()

    @pl.when((i > 0) & (i < n_blocks))
    def _():
        finish()
        project()

    @pl.when(i == n_blocks)
    def _():
        finish()


def q_latent(dp_index, normed, w_qa, gain_q, w_out, chunks, piece_rows):
    rows, depth = normed.shape
    rank = w_qa.shape[1]
    n_blocks = rows // BLOCK
    total = sum(chunks) // PIECE

    def piece_spec(first, count):
        return pl.BlockSpec((piece_rows, PIECE), lambda i, ids: (0, jnp.clip(i - first, 0, count - 1)))

    firsts = [sum(chunks[:j]) // PIECE for j in range(len(chunks))]
    return pl.pallas_call(
        functools.partial(q_latent_kernel, n_blocks, chunks),
        grid_spec=pltpu.PrefetchScalarGridSpec(
            num_scalar_prefetch=1,
            grid=(n_blocks + 1,),
            in_specs=[
                pl.BlockSpec((BLOCK, depth), lambda i, ids: (jnp.minimum(i, n_blocks - 1), 0)),
                whole(w_qa),
                whole(gain_q),
                pl.BlockSpec((piece_rows, PIECE), lambda i, ids: (ids[0], jnp.minimum(i, total - 1))),
            ],
            out_specs=[pl.BlockSpec((BLOCK, rank), lambda i, ids: (jnp.maximum(i - 1, 0), 0))] + [piece_spec(f, c // PIECE) for f, c in zip(firsts, chunks)],
            scratch_shapes=[pltpu.VMEM((2, BLOCK, rank), F32)],
        ),
        out_shape=[jax.ShapeDtypeStruct((rows, rank), BF16)] + [jax.ShapeDtypeStruct((piece_rows, c), F32) for c in chunks],
        compiler_params=pltpu.CompilerParams(vmem_limit_bytes=VMEM_LIMIT),
        cost_estimate=pl.CostEstimate(flops=2 * rows * depth * rank, bytes_accessed=rows * depth * 2, transcendentals=0),
        name='q_latent',
    )(dp_index, normed, w_qa, gain_q, w_out)


def attn_kernel(n_seq, cq_ref, c_ref, kre_ref, kro_ref, wq_ref, wkv_ref, cos_ref, sin_ref, o_ref, s_ref, qa, kva, qb, kvb, *cast):
    if cast:
        wq, wkv = cast
        wq[...] = wq_ref[...].astype(BF16)
        wkv[...] = wkv_ref[...].astype(BF16)
    else:
        wq, wkv = wq_ref, wkv_ref

    def projections(b, q_scr, kv_scr):
        rows = pl.ds(pl.multiple_of(b * SEQ, SEQ), SEQ)

        def even_nope():
            q = dot(cq_ref[rows, :], jnp.concatenate([wq[:, 0:128], wq[:, 384:512]], axis=1)).astype(BF16)
            q_scr[:, 0:256] = q

        def odd_and_rope(at):
            q = dot(cq_ref[rows, :], wq[:, at + 128:at + 384])
            t1, t2 = q[:, :128], q[:, 128:]
            low = lax.broadcasted_iota(jnp.int32, t1.shape, 1) < ROPE
            rope = rotate_pairs(jnp.where(low, t1, t2), cos_ref[...], sin_ref[...])
            nope = pltpu.roll(jnp.where(low, t2, t1), 64, 1)
            first_col = 256 + at // 384 * 256
            q_scr[:, first_col:first_col + 256] = jnp.concatenate([rope, nope], axis=1).astype(BF16)

        def keys_values(heads):
            for h in heads:
                kv_scr[:, 256 * h:256 * h + 256] = dot(c_ref[rows, :], wkv[:, 256 * h:256 * h + 256]).astype(BF16)

        return [even_nope, lambda: odd_and_rope(0), lambda: odd_and_rope(384), lambda: keys_values((0, 1)), lambda: keys_values((2, 3))]

    def attention(b, q_scr, kv_scr):
        start = pl.multiple_of(b * SEQ, SEQ)
        rows = pl.ds(start, SEQ)
        keep = lax.broadcasted_iota(jnp.int32, (HALF, HALF), 0) >= lax.broadcasted_iota(jnp.int32, (HALF, HALF), 1)
        factor = LOGIT_SCALE * LOG2E

        def logits(h):
            at = 256 + 256 * (h // 2)
            k_nope = kv_scr[:, 256 * h:256 * h + 128]
            if h % 2 == 0:
                q = jnp.concatenate([q_scr[:, 64 * h:64 * h + 128], q_scr[:, at:at + 128]], axis=1)
                k = jnp.concatenate([k_nope, kre_ref[rows, :]], axis=1)
            else:
                q = q_scr[:, at:at + 256]
                k = jnp.concatenate([kro_ref[rows, :], k_nope], axis=1)
            return dot_nt(q, k[:HALF]), dot_nt(q[HALF:], k[HALF:])

        def softmax(left, right):
            top = jnp.where(keep, left[:HALF], -jnp.inf)
            low_l = left[HALF:]
            low_r = jnp.where(keep, right, -jnp.inf)
            m0 = jnp.max(top, axis=1, keepdims=True)
            e0 = jnp.exp2((top - m0) * factor)
            p0 = (e0 * (1.0 / jnp.sum(e0, axis=1, keepdims=True))).astype(BF16)
            m1 = jnp.max(jnp.maximum(low_l, low_r), axis=1, keepdims=True)
            e1 = jnp.exp2((low_l - m1) * factor)
            e2 = jnp.exp2((low_r - m1) * factor)
            inv = 1.0 / jnp.sum(e1 + e2, axis=1, keepdims=True)
            biggest = jnp.max(jnp.maximum(m0, m1).reshape(HALF // 8, 8, 1), axis=0)
            return jnp.concatenate([p0, (e1 * inv).astype(BF16)], axis=0), (e2 * inv).astype(BF16), biggest

        def values(h, p_left, p_right, _):
            v = kv_scr[:, 256 * h + 128:256 * h + 256]
            o_left = dot(p_left, v[:HALF])
            return o_left[:HALF], o_left[HALF:] + dot(p_right, v[HALF:])

        def store(h, even, odd):
            cols = slice(128 * h, 128 * h + 256)
            o_ref[pl.ds(start, HALF), cols] = jnp.concatenate([even[0], odd[0]], axis=1).astype(BF16)
            o_ref[pl.ds(pl.multiple_of(start + HALF, HALF), HALF), cols] = jnp.concatenate([even[1], odd[1]], axis=1).astype(BF16)

        return logits, softmax, values, store

    def step(b, held, nxt, spare, maxima):
        logits, softmax, values, store = attention(b, *held)
        parts = [lambda: None] * 5 if spare is None else projections(nxt, *spare)
        l0 = logits(0)
        parts[0]()
        l1 = logits(1)
        p0 = softmax(*l0)
        parts[1]()
        o0 = values(0, *p0)
        l2 = logits(2)
        p1 = softmax(*l1)
        parts[2]()
        store(0, o0, values(1, *p1))
        l3 = logits(3)
        p2 = softmax(*l2)
        parts[3]()
        o2 = values(2, *p2)
        p3 = softmax(*l3)
        parts[4]()
        store(2, o2, values(3, *p3))
        return tuple(jnp.maximum(m, p[2]) for m, p in zip(maxima, (p0, p1, p2, p3)))

    slot_a, slot_b = (qa, kva), (qb, kvb)
    maxima = tuple(jnp.full((8, 1), -jnp.inf, F32) for _ in range(GROUP))
    for part in projections(0, *slot_a):
        part()

    def body(i, maxima):
        maxima = step(2 * i, slot_a, 2 * i + 1, slot_b, maxima)
        return step(2 * i + 1, slot_b, jnp.minimum(2 * i + 2, n_seq - 1), slot_a, maxima)

    maxima = lax.fori_loop(0, n_seq // 2, body, maxima)
    if n_seq % 2:
        maxima = step(n_seq - 1, slot_a, None, None, maxima)
    s_ref[0] = jnp.concatenate([jnp.broadcast_to(m * LOGIT_SCALE, (8, 128)) for m in maxima], axis=0)


def attend_heads(c_q, c_kv, kr_even, kr_odd, w_q, w_kv, cos, sin):
    tokens = c_q.shape[0]
    heads = w_q.shape[1] // (NOPE + ROPE)
    groups = heads // GROUP
    q_cols, kv_cols = GROUP * (NOPE + ROPE), GROUP * (NOPE + VDIM)
    scratch = [pltpu.VMEM((SEQ, q_cols), BF16), pltpu.VMEM((SEQ, kv_cols), BF16)] * 2
    if w_q.dtype != BF16:
        scratch += [pltpu.VMEM((w_q.shape[0], q_cols), BF16), pltpu.VMEM((w_kv.shape[0], kv_cols), BF16)]
    flops = 2 * tokens * heads * (w_q.shape[0] * 192 + w_kv.shape[0] * 256 + SEQ * 256)
    out, top = pl.pallas_call(
        functools.partial(attn_kernel, tokens // SEQ),
        grid=(groups,),
        in_specs=[whole(c_q), whole(c_kv), whole(kr_even), whole(kr_odd), pl.BlockSpec((w_q.shape[0], q_cols), lambda g: (0, g)), pl.BlockSpec((w_kv.shape[0], kv_cols), lambda g: (0, g)), whole(cos), whole(sin)],
        out_specs=[pl.BlockSpec((tokens, GROUP * VDIM), lambda g: (0, g)), pl.BlockSpec((1, 8 * GROUP, 128), lambda g: (g, 0, 0))],
        out_shape=[jax.ShapeDtypeStruct((tokens, heads * VDIM), BF16), jax.ShapeDtypeStruct((groups, 8 * GROUP, 128), F32)],
        scratch_shapes=scratch,
        compiler_params=pltpu.CompilerParams(vmem_limit_bytes=VMEM_LIMIT),
        cost_estimate=pl.CostEstimate(flops=flops, bytes_accessed=tokens * heads * VDIM * 2, transcendentals=tokens * heads * SEQ),
    )(c_q, c_kv, kr_even, kr_odd, w_q, w_kv, cos, sin)
    return out, jnp.max(top.reshape(heads, 8, 128)[:, :, 0], axis=1)


def out_kernel(n_cols, first_col, n_recv, recv_col, tp_ref, o_own, o_far, w_own, w_far, x_hbm, *rest):
    extra = (first_col > 0) + (n_recv > 0)
    recv = rest[extra - 1] if n_recv else None
    y_hbm, send, own_buf, far_buf, wo_buf, wf_buf, x_buf, y_buf, t_buf, o_sem, w_sem, x_sem, y_sem, t_sem = rest[extra:extra + 14]
    if n_recv:
        r_buf, rx_buf, ry_buf, r_sem, ry_sem = rest[extra + 14:]
    tp_at = tp_ref[0]
    n_rows = o_own.shape[0] // BM
    parts = BM // 128
    s = pl.program_id(0)
    steps = n_rows * n_cols
    m, n = s // n_cols, s % n_cols
    slot = s % 2

    def o_copies(m, part, size):
        rows = pl.ds(pl.multiple_of(m * BM + part * 128, 128), size)
        inner = pl.ds(part * 128, size)
        return [pltpu.make_async_copy(src.at[rows, :], dst.at[m % 2, inner, :], o_sem.at[k, m % 2]) for k, (src, dst) in enumerate(((o_own, own_buf), (o_far, far_buf)))]

    def y_rows(s):
        return pl.ds(pl.multiple_of(s // n_cols * BM + tp_at * SEQ, 128), BM)

    def y_cols(s):
        return pl.ds(pl.multiple_of(first_col + s % n_cols * BN, BN), BN)

    def w_copies(s):
        k = s % 2
        return [
            pltpu.make_async_copy(w_own.at[:, y_cols(s)], wo_buf.at[k], w_sem.at[0, k]),
            pltpu.make_async_copy(w_far.at[:, pl.ds(pl.multiple_of(s % n_cols * BN, BN), BN)], wf_buf.at[k], w_sem.at[1, k]),
            pltpu.make_async_copy(x_hbm.at[y_rows(s), y_cols(s)], x_buf.at[k], x_sem.at[k]),
        ]

    def y_copy(s):
        return pltpu.make_async_copy(y_buf.at[s % 2], y_hbm.at[y_rows(s), y_cols(s)], y_sem.at[s % 2])

    def t_copy(n):
        inner = pl.multiple_of(tp_at * (BM - SEQ), 128)
        return pltpu.make_async_copy(t_buf.at[n % 2, pl.ds(inner, SEQ), :], send.at[:, pl.ds(pl.multiple_of(n * BN, BN), BN)], t_sem.at[n % 2])

    other_rows = pl.ds(pl.multiple_of((1 - tp_at) * (x_hbm.shape[0] - SEQ), SEQ), SEQ)

    def r_copies(s):
        k = s % 2
        return [
            pltpu.make_async_copy(recv.at[:, pl.ds(pl.multiple_of(s * BN, BN), BN)], r_buf.at[k], r_sem.at[0, k]),
            pltpu.make_async_copy(x_hbm.at[other_rows, pl.ds(pl.multiple_of(recv_col + s * BN, BN), BN)], rx_buf.at[k], r_sem.at[1, k]),
        ]

    def ry_copy(s):
        return pltpu.make_async_copy(ry_buf.at[s % 2], y_hbm.at[other_rows, pl.ds(pl.multiple_of(recv_col + s * BN, BN), BN)], ry_sem.at[s % 2])

    @pl.when(s == 0)
    def _():
        first = w_copies(0) + o_copies(0, 0, BM)
        for copy in first:
            copy.start()
        for copy in first:
            copy.wait()

    @pl.when(s + 1 < steps)
    def _():
        for copy in w_copies(s + 1):
            copy.start()

    for part in range(parts):
        @pl.when((n == part * n_cols // parts) & (m + 1 < n_rows))
        def _(part=part):
            for copy in o_copies(m + 1, part, 128):
                copy.start()

    if n_recv:
        @pl.when(s == 0)
        def _():
            for copy in r_copies(0):
                copy.start()

        @pl.when(s + 1 < n_recv)
        def _():
            for copy in r_copies(s + 1):
                copy.start()

        @pl.when(s < n_recv)
        def _():
            for copy in r_copies(s):
                copy.wait()

        @pl.when((s >= 2) & (s - 2 < n_recv))
        def _():
            ry_copy(s - 2).wait()

    @pl.when((n == 0) & (m > 0))
    def _():
        for copy in o_copies(m, 0, BM):
            copy.wait()

    @pl.when(s >= 2)
    def _():
        y_copy(s - 2).wait()

    exclusive = m == tp_at * (n_rows - 1)

    @pl.when(exclusive & (n >= 2))
    def _():
        t_copy(n - 2).wait()

    @pl.when(s > 0)
    def _():
        for copy in w_copies(s):
            copy.wait()

    total = dot(own_buf[m % 2], wo_buf[slot]) + dot(far_buf[m % 2], wf_buf[slot].astype(BF16))
    t_buf[n % 2] = total
    y_buf[slot] = (x_buf[slot].astype(F32) + total).astype(BF16)
    if n_recv:
        ry_buf[slot] = (rx_buf[slot].astype(F32) + r_buf[slot]).astype(BF16)
    y_copy(s).start()

    @pl.when(exclusive)
    def _():
        t_copy(n).start()

    @pl.when(exclusive & (n == n_cols - 1))
    def _():
        for k in range(max(0, n_cols - 2), n_cols):
            t_copy(k).wait()

    if n_recv:
        @pl.when(s < n_recv)
        def _():
            ry_copy(s).start()

    @pl.when(s == steps - 1)
    def _():
        y_copy(s - 1).wait()
        y_copy(s).wait()
        if n_recv > steps - 2:
            for k in range(steps - 2, n_recv):
                ry_copy(k).wait()


def project_out(tp_index, o_own, o_far, w_own, w_far, hidden, previous, first_col, received, recv_col):
    rows, depth = o_own.shape
    cols = w_far.shape[1]
    n_cols = cols // BN
    n_recv = 0 if received is None else received.shape[1] // BN
    extra = [a for a in (previous, received) if a is not None]
    scratch = [
        pltpu.VMEM((2, BM, depth), BF16),
        pltpu.VMEM((2, BM, depth), BF16),
        pltpu.VMEM((2, depth, BN), BF16),
        pltpu.VMEM((2, depth, BN), F32),
        pltpu.VMEM((2, BM, BN), BF16),
        pltpu.VMEM((2, BM, BN), BF16),
        pltpu.VMEM((2, BM, BN), F32),
        pltpu.SemaphoreType.DMA((2, 2)),
        pltpu.SemaphoreType.DMA((2, 2)),
        pltpu.SemaphoreType.DMA((2,)),
        pltpu.SemaphoreType.DMA((2,)),
        pltpu.SemaphoreType.DMA((2,)),
    ]
    if n_recv:
        scratch += [pltpu.VMEM((2, SEQ, BN), F32), pltpu.VMEM((2, SEQ, BN), BF16), pltpu.VMEM((2, SEQ, BN), BF16), pltpu.SemaphoreType.DMA((2, 2)), pltpu.SemaphoreType.DMA((2,))]
    return pl.pallas_call(
        functools.partial(out_kernel, n_cols, first_col, n_recv, recv_col),
        grid_spec=pltpu.PrefetchScalarGridSpec(
            num_scalar_prefetch=1,
            grid=(rows // BM * n_cols,),
            in_specs=[pl.BlockSpec(memory_space=pl.ANY)] * (5 + len(extra)),
            out_specs=[pl.BlockSpec(memory_space=pl.ANY)] * 2,
            scratch_shapes=scratch,
        ),
        out_shape=[jax.ShapeDtypeStruct(hidden.shape, BF16), jax.ShapeDtypeStruct((SEQ, cols), F32)],
        input_output_aliases={} if previous is None else {6: 0},
        compiler_params=pltpu.CompilerParams(vmem_limit_bytes=VMEM_LIMIT),
        cost_estimate=pl.CostEstimate(flops=4 * rows * depth * cols, bytes_accessed=rows * depth * 4, transcendentals=0),
    )(tp_index, o_own, o_far, w_own, w_far, hidden, *extra)


def rescale_kernel(wq_ref, wkv_ref, gq_ref, gkv_ref, nq_ref, nkv_ref):
    nq_ref[...] = (wq_ref[...].astype(F32) * gq_ref[...]).astype(BF16)
    nkv_ref[...] = (wkv_ref[...].astype(F32) * gkv_ref[...]).astype(BF16)


def rescale(w_qb, w_kvb, gain_qb, gain_kvb):
    steps = 8
    blocks = [pl.BlockSpec((w.shape[0] // steps, w.shape[1]), lambda i: (i, 0)) for w in (w_qb, w_kvb)]
    return pl.pallas_call(
        rescale_kernel,
        grid=(steps,),
        in_specs=blocks + [whole(gain_qb), whole(gain_kvb)],
        out_specs=blocks,
        out_shape=[jax.ShapeDtypeStruct(w.shape, BF16) for w in (w_qb, w_kvb)],
        compiler_params=pltpu.CompilerParams(vmem_limit_bytes=VMEM_LIMIT),
        cost_estimate=pl.CostEstimate(flops=2 * (w_qb.size + w_kvb.size), bytes_accessed=4 * (w_qb.size + w_kvb.size), transcendentals=0),
        name='rescale',
    )(w_qb, w_kvb, gain_qb, gain_kvb)


def column_gains(first_gain, first_dim, second_gain, second_dim):
    num_heads = first_gain.shape[0]
    return jnp.concatenate([jnp.broadcast_to(first_gain[:, None], (num_heads, first_dim)), jnp.broadcast_to(second_gain[:, None], (num_heads, second_dim))], axis=1).reshape(-1)


def solution(mesh):
    tp, dp = mesh.shape['tp'], mesh.shape['dp']
    swap = [(i, (i + 1) % tp) for i in range(tp)]

    def cross(piece):
        return lax.ppermute(piece, 'tp', swap)

    def far_piece(weight):
        rows = weight.shape[0] // dp
        return cross(lax.dynamic_slice_in_dim(weight, lax.axis_index('dp') * rows, rows, 0).astype(F32))

    def gather(piece):
        return lax.all_gather(piece, 'dp', axis=0, tiled=True)

    def device_step(hidden, gain_in, gain_q, gain_kv, w_qa, w_kva, w_qb, w_kvb, w_out):
        num_seqs, seq_len, model_dim = hidden.shape
        heads = w_out.shape[0] // VDIM
        tp_at = lax.axis_index('tp').astype(jnp.int32)
        flat = hidden.reshape(num_seqs * seq_len, model_dim)
        starts = [sum(COLUMN_CHUNKS[:i]) for i in range(len(COLUMN_CHUNKS))]

        kvb_piece = far_piece(w_kvb)
        qb_piece = far_piece(w_qb)
        cos, sin = rope_tables(ROPE)
        normed, c_kv, kr_even, kr_odd = kv_latent(tp_at[None], flat, gain_in[None], w_kva.T, gain_kv[None], cos, sin, num_seqs - tp + 1)
        normed, kvb_piece = lax.optimization_barrier((normed, kvb_piece))
        far_kvb = gather(kvb_piece)
        dp_index = lax.axis_index('dp').astype(jnp.int32)[None]
        c_q, *out_pieces = q_latent(dp_index, normed, w_qa, gain_q[None], w_out, COLUMN_CHUNKS, w_out.shape[0] // dp)
        out_pieces = [cross(piece) for piece in out_pieces]
        c_q, qb_piece = lax.optimization_barrier((c_q, qb_piece))
        far_qb = gather(qb_piece)
        latents = (c_q, c_kv, kr_even, kr_odd)
        o_own, top_own = attend_heads(*latents, w_qb, w_kvb, cos, sin)
        o_own, *ready = lax.optimization_barrier((o_own, *out_pieces[:2]))
        far_out = [gather(piece) for piece in ready]
        o_far, top_far = attend_heads(*latents, far_qb, far_kvb, cos, sin)
        o_far, *ready = lax.optimization_barrier((o_far, *out_pieces[2:]))
        far_out += [gather(piece) for piece in ready]

        head_at = tp_at * heads
        top = jnp.zeros((tp * heads,), F32)
        top = lax.dynamic_update_slice(top, top_own, (head_at,))
        top = lax.dynamic_update_slice(top, top_far, (heads - head_at,))
        hops = [('tp', swap)] + [('dp', [(i, i ^ (1 << bit)) for i in range(dp)]) for bit in range(dp.bit_length() - 1)]

        other_row = (1 - tp_at) * (num_seqs - 1) * seq_len

        def receive(y, part, first_col):
            cols = part.shape[1]
            rows = lax.dynamic_slice(flat, (other_row, first_col), (seq_len, cols)).astype(F32)
            return lax.dynamic_update_slice(y, (rows + part).astype(BF16), (other_row, first_col))

        y = None
        arriving = []
        for i, (s, w_far) in enumerate(zip(starts, far_out)):
            if i < len(hops):
                hopped = lax.ppermute(top, *hops[i])
            received, recv_col = arriving.pop(0) if i > 1 else (None, 0)
            y, part = project_out(tp_at[None], o_own, o_far, w_out, w_far, flat, y, s, received, recv_col)
            if i < len(hops):
                y, top, hopped = lax.optimization_barrier((y, top, hopped))
                top = jnp.maximum(top, hopped)
            arriving.append((lax.ppermute(part, 'tp', swap), s))

        logit_max = top
        own_max = lax.dynamic_slice(logit_max, (head_at,), (heads,))
        clip_gain = CLIP_TAU / jnp.maximum(CLIP_TAU, own_max)
        root_gain = jnp.sqrt(clip_gain)
        gain_qb = column_gains(root_gain, NOPE, clip_gain, ROPE)[None]
        gain_kvb = column_gains(root_gain, NOPE, jnp.ones_like(clip_gain), VDIM)[None]
        y, gain_qb, gain_kvb = lax.optimization_barrier((y, gain_qb, gain_kvb))
        new_qb, new_kvb = rescale(w_qb, w_kvb, gain_qb, gain_kvb)
        for part, s in arriving:
            y = receive(y, part, s)
        return y.reshape(hidden.shape), logit_max, new_qb, new_kvb

    weight_spec = P(None, 'tp')
    return jax.shard_map(device_step, mesh=mesh, in_specs=(P('dp', None, None), P(), P(), P(), P(), P(), weight_spec, weight_spec, P('tp', None)), out_specs=(P('dp', None, None), P(), weight_spec, weight_spec), check_vma=False)
```
